256 devices in a mesh: dp: 16 (over x, z_lo), cls: 16 (over y, z_hi, core).
Axes of the slice: x: 4, y: 4, z: 8 (z_hi: 2, z_lo: 4; z = z_hi * 4 + z_lo), core: 2. Of those that a mesh axis runs over, the one named last changes fastest.
Arguments:
- embeddings: bfloat16 [49152, 768], P('dp'), may hold values from -6 to 6
- labels: int32 [49152], P('dp'), may hold values from 0 to 22015, as said below
- row_count: int32 [16], P('dp'), may hold values from 768 to 3072
Outputs:
- class_means: float32 [22016, 768], P(('dp', 'cls'))
- prototypes: float32 [22016, 768], P(('dp', 'cls'))
- similarity: float32 [49152], P('dp')
The draws below stay inside these ranges and needn't reach their ends.
Inputs may be any that keep to these rules, and one draw needn't show every extreme that they name: Rows of index i of dp at or beyond row_count[i] are padding. `labels`: classes c and c' belong to the same block when c // 86 == c' // 86; block b belongs to index b mod 16 of cls. The rows of one index of dp name at most 16 distinct classes of any one block. Some block has exactly 16 of its classes named by the rows of every index of dp. The rows of some index of dp name exactly 16 classes of every block of some index of cls.
All inputs are finite; a program needn't handle non-finite values.
Results may differ from the reference program's by a relative error of at most 0.0017.
Values sent between devices are 32-bit elements; how exact they have to be, the bound alone decides.
A program may use at most 64 MiB of HBM per device.

```python
import jax
import jax.numpy as jnp
from jax import lax

D = 768
CLS_DEV = 86
SLOTS = 16
ROWS_DEV = 3072
CLASSES = 22016
ROWS = 49152
N_DP = 16


def draw_labels(key, part):
    blocks = ROWS // ROWS_DEV
    owners = CLASSES // CLS_DEV
    group_count = owners // blocks
    keys = jax.random.split(jax.random.fold_in(key, 17), 7)
    class_iota = jnp.arange(CLS_DEV, dtype=jnp.int32)
    scores = jax.random.randint(keys[0], (blocks, owners, CLS_DEV), 0, 1 << 20) * CLS_DEV + class_iota
    allowed = jnp.argsort(scores, axis=2)[:, :, :SLOTS].astype(jnp.int32)
    owner_scores = jax.random.randint(keys[1], (owners,), 0, 1 << 20) * owners + jnp.arange(owners, dtype=jnp.int32)
    owner_order = jnp.argsort(owner_scores).astype(jnp.int32)
    first_pick = jax.random.randint(keys[2], (blocks, ROWS_DEV), 0, owners)
    second_pick = jax.random.randint(keys[3], (blocks, ROWS_DEV), 0, owners)
    owner_rank = jnp.minimum(first_pick, second_pick).astype(jnp.int32)
    slot_first = jax.random.randint(keys[4], (blocks, ROWS_DEV), 0, SLOTS)
    slot_second = jax.random.randint(keys[5], (blocks, ROWS_DEV), 0, SLOTS)
    slot = jnp.minimum(slot_first, slot_second).astype(jnp.int32)
    position = jnp.broadcast_to(jnp.arange(ROWS_DEV, dtype=jnp.int32)[None, :], (blocks, ROWS_DEV))
    block_index = jnp.broadcast_to(jnp.arange(blocks, dtype=jnp.int32)[:, None], (blocks, ROWS_DEV))
    forced = position < SLOTS
    owner_rank = jnp.where(forced, 0, owner_rank)
    slot = jnp.where(forced, position, slot)
    chosen_owner = owner_order[owner_rank].astype(jnp.int32)
    full_sender = jax.random.randint(keys[6], (), 0, blocks).astype(jnp.int32)
    base_group = (owner_order[0] % group_count).astype(jnp.int32)
    widened = (block_index == full_sender) & (position < blocks * SLOTS)
    wide_owner = (base_group + group_count * (position // SLOTS)).astype(jnp.int32)
    chosen_owner = jnp.where(widened, wide_owner, chosen_owner).astype(jnp.int32)
    slot = jnp.where(widened, position % SLOTS, slot).astype(jnp.int32)
    local_class = allowed[block_index, chosen_owner, slot]
    labels = chosen_owner * CLS_DEV + local_class
    return labels.reshape(ROWS).astype(jnp.int32)


def set_ends(entries, key, smallest, largest):
    place = [jax.random.randint(jax.random.fold_in(key, axis), (), 0, length) for axis, length in enumerate(entries.shape)]
    widest = entries.shape.index(max(entries.shape))
    neighbour = place[:widest] + [(place[widest] + 1) % entries.shape[widest]] + place[widest + 1:]
    return entries.at[tuple(place)].set(smallest).at[tuple(neighbour)].set(largest)


def level_of(stream_key, shape, cuts, smallest, top_value):
    gain, own = 1.0, jax.random.fold_in(stream_key, 6)
    for axis_at, shards_of in cuts:
        heights = jnp.exp(jax.random.uniform(jax.random.fold_in(own, axis_at), (shards_of,), jnp.float32, smallest / len(cuts), top_value / len(cuts)))
        gain = gain * jnp.repeat(heights, shape[axis_at] // shards_of).reshape([-1 if axis == axis_at else 1 for axis in range(len(shape))])
    return gain


def bell_draw(rng, extent, deviation, reach, cuts=(), held_as=jnp.bfloat16):
    array = jax.random.normal(rng, extent, jnp.float32) * deviation
    if len(cuts) > 0:
        array = level_of(rng, extent, cuts, -0.22, 0.18) * array
    return jnp.clip(array, min=-reach, max=reach).astype(held_as)


def setup_inputs(seed: int = 0) -> dict:
    splits = jax.random.split(jax.random.key(seed), 4)
    embeddings = bell_draw(splits[0], (ROWS, D), 1.0, 6.0, ((0, 16),))
    labels = draw_labels(jax.random.fold_in(splits[3], 71), 0)
    row_count = set_ends(jax.random.randint(splits[2], (N_DP,), max(ROWS_DEV // 4, N_DP * SLOTS), ROWS_DEV + 1), jax.random.fold_in(splits[2], 1), max(ROWS_DEV // 4, N_DP * SLOTS), ROWS_DEV).astype(jnp.int32)
    return dict(embeddings=embeddings, labels=labels, row_count=row_count)


epsilon = 1e-06
sharpness = 4.0

def normalize(matrix):
    return matrix / jnp.sqrt(lax.optimization_barrier(jnp.sum(matrix * matrix, axis=1, keepdims=True)) + epsilon)

def reference(embeddings, labels, row_count):
    row_total = embeddings.shape[0]
    position = jnp.arange(row_total, dtype=jnp.int32)
    owner = (position // ROWS_DEV).astype(jnp.int32)
    alive = (position % ROWS_DEV < row_count[owner]).astype(jnp.float32)
    features = embeddings.astype(jnp.float32)
    class_sums = jax.ops.segment_sum(features * alive[:, None], labels, num_segments=CLASSES)
    counts = jax.ops.segment_sum(alive, labels, num_segments=CLASSES)
    class_means = class_sums / jnp.maximum(counts, 1.0)[:, None]
    unit_rows = normalize(class_means)
    lengths = jnp.sqrt(lax.optimization_barrier(jnp.sum(features * features, axis=1)) + epsilon)
    similarity = alive * lax.optimization_barrier(jnp.sum(features * unit_rows[labels], axis=1)) / lengths
    weight = (alive * jnp.exp(sharpness * (similarity - 1.0))).astype(jnp.bfloat16).astype(jnp.float32)
    weighted = jax.ops.segment_sum(features * weight[:, None], labels, num_segments=CLASSES)
    prototypes = normalize(weighted)
    return (class_means, prototypes, similarity)
```

```python
import jax
import jax.numpy as jnp
from jax import lax
from jax.experimental import pallas as pl
from jax.experimental.pallas import tpu as pltpu
from jax.sharding import PartitionSpec as P

MESH = pl.DeviceIdType.MESH
F32 = jnp.float32
BF16 = jnp.bfloat16

CLS_DEV = 86
SLOTS = 16
PEERS = 16
TABLE = PEERS * SLOTS
LANES = 128
EPSILON = 1e-06
SHARPNESS = 4.0

X, Y, Z = 4, 4, 8
DX = [k // 4 for k in range(PEERS)]
DZ = [(0, 1, -1, 2)[k % 4] for k in range(PEERS)]


def split(value, parts):
    pieces, rest = [], value
    for number in range(parts):
        piece = rest.astype(BF16)
        pieces.append(piece)
        if number < parts - 1:
            rest = rest - piece.astype(F32)
    return pieces


def dot(a, b, contract):
    return lax.dot_general(a, b, (contract, ((), ())), preferred_element_type=F32)


NN = ((1,), (0,))
NT = ((1,), (1,))
TN = ((0,), (0,))


def ranks(present):
    before = lax.broadcasted_iota(jnp.int32, (LANES, LANES), 0)
    after = lax.broadcasted_iota(jnp.int32, (LANES, LANES), 1)
    triangle = jnp.where(before < after, 1.0, 0.0).astype(BF16)
    return dot(present.astype(BF16), triangle, NN)


def kernel(
    rc_ref,
    lab_ref,
    e_hbm,
    means_ref,
    proto_ref,
    sim_ref,
    e_ref,
    hot_ref,
    meta_out,
    meta_in,
    out1,
    in1,
    out2,
    in2,
    out3,
    in3,
    map_ref,
    part_ref,
    sim_own,
    sim_in,
    sim_half,
    sim_far,
    e_sem,
    meta_ssem,
    meta_rsem,
    ssem,
    rsem,
    sim_ssem,
    sim_rsem,
):
    rows, width = e_ref.shape
    dp, cls = lax.axis_index("dp"), lax.axis_index("cls")
    x, z_lo = dp // 4, dp % 4
    y, z_hi, core = cls // 4, (cls // 2) % 2, cls % 2
    z = z_hi * 4 + z_lo
    sign = 1 - 2 * core

    def device(x_at, y_at, z_at, core_at):
        return (x_at * 4 + z_at % 4, y_at * 4 + (z_at // 4) * 2 + core_at)

    def at_offset(dx, dz):
        return device((x + X + sign * dx) % X, y, (z + Z + sign * dz) % Z, core)

    fan = [(dy, dc) for dc in range(2) for dy in range(Y) if (dy, dc) != (0, 0)]

    def fan_device(dy, dc):
        return device(x, (y + dy) % Y, z, (core + dc) % 2)

    far = device(x, y, (z + 4) % Z, core)

    pieces = e_sem.shape[0]
    piece_rows = rows // pieces
    loads = [
        pltpu.make_async_copy(
            e_hbm.at[pl.ds(n * piece_rows, piece_rows)],
            e_ref.at[pl.ds(n * piece_rows, piece_rows)],
            e_sem.at[n],
        )
        for n in range(pieces)
    ]
    for load in loads:
        load.start()

    barrier = pltpu.get_barrier_semaphore()
    greeted = 0
    for dx in range(X):
        for dz in range(-2, 3):
            if (dx, dz) != (0, 0):
                pl.semaphore_signal(barrier, inc=1, device_id=at_offset(dx, dz), device_id_type=MESH)
                greeted += 1
    for dy, dc in fan:
        pl.semaphore_signal(barrier, inc=1, device_id=fan_device(dy, dc), device_id_type=MESH)
        greeted += 1
    pl.semaphore_signal(barrier, inc=1, device_id=far, device_id_type=MESH)
    greeted += 1

    label = lab_ref[...]
    position = lax.broadcasted_iota(jnp.int32, (1, rows), 1)
    block = (label * 48771) >> 22
    inner = label - block * CLS_DEV
    block_dp, block_cls = block >> 4, block & 15
    block_z = ((block_cls >> 1) & 1) * 4 + (block_dp & 3)
    dx = ((block_dp >> 2) - x) * sign & 3
    dz = (block_z - z) * sign & 7
    turn = jnp.where(dz == 7, 2, jnp.where(dz == 2, 3, dz))
    owned = (
        (position < rc_ref[0])
        & ((block_cls >> 2) == y)
        & ((block_cls & 1) == core)
        & ((dz <= 2) | (dz == 7))
    )
    peer = jnp.where(owned, dx * 4 + turn, -1)
    peer_iota = lax.broadcasted_iota(jnp.int32, (PEERS, rows), 0)
    inner_iota = lax.broadcasted_iota(jnp.int32, (LANES, rows), 0)
    peer_hot = jnp.where(peer == peer_iota, 1.0, 0.0)
    inner_hot = jnp.where(inner == inner_iota, 1.0, 0.0).astype(BF16)
    counts = dot(peer_hot.astype(BF16), inner_hot, NT)
    rank = ranks(jnp.where(counts > 0, 1.0, 0.0))
    ranked = dot(rank.astype(BF16), inner_hot, NN)
    rank_row = jnp.sum(peer_hot * ranked, axis=0, keepdims=True)
    slot = jnp.where(owned, peer * SLOTS + rank_row.astype(jnp.int32), -1)

    for k in range(PEERS):
        meta_out[k] = jnp.broadcast_to(counts[k : k + 1], (8, LANES))
    meta_in[0] = jnp.broadcast_to(counts[0:1], (8, LANES))

    slot_iota = lax.broadcasted_iota(jnp.int32, (TABLE, rows), 0)
    hot_ref[...] = jnp.where(slot == slot_iota, 1.0, 0.0).astype(BF16)

    pl.semaphore_wait(barrier, greeted)
    metas = {}
    for k in range(1, PEERS):
        metas[k] = pltpu.make_async_remote_copy(
            src_ref=meta_out.at[k],
            dst_ref=meta_in.at[k],
            send_sem=meta_ssem.at[k],
            recv_sem=meta_rsem.at[k],
            device_id=at_offset(DX[k], DZ[k]),
            device_id_type=MESH,
        )
        metas[k].start()

    def exchange(phase, source, target, back):
        copies = []
        for k in range(1, PEERS):
            to = at_offset(-DX[k], -DZ[k]) if back else at_offset(DX[k], DZ[k])
            copy = pltpu.make_async_remote_copy(
                src_ref=source.at[pl.ds(k * SLOTS, SLOTS)],
                dst_ref=target.at[pl.ds(k * SLOTS, SLOTS)],
                send_sem=ssem.at[phase, k],
                recv_sem=rsem.at[phase, k],
                device_id=to,
                device_id_type=MESH,
            )
            copy.start()
            copies.append(copy)
        return copies

    for load in loads:
        load.wait()
    out1[...] = dot(hot_ref[...], e_ref[...], NN)
    in1[pl.ds(0, SLOTS)] = out1[pl.ds(0, SLOTS)]
    sends1 = exchange(0, out1, in1, False)

    ones = jnp.ones((8, LANES), BF16)
    step = 512
    for n in range(rows // step):
        tile = e_ref[pl.ds(n * step, step), :].astype(F32)
        squares = tile * tile
        lanes = squares[:, 0:LANES]
        for j in range(1, width // LANES):
            lanes = lanes + squares[:, j * LANES : (j + 1) * LANES]
        total = sum(dot(ones, piece, NT) for piece in split(lanes, 3))
        part_ref[0:1, pl.ds(n * step, step)] = total[0:1]

    for k in range(1, PEERS):
        metas[k].wait()
    counts8 = meta_in[...].reshape(PEERS * 8, LANES)
    present8 = counts8 > 0
    rank8 = jnp.where(present8, ranks(jnp.where(present8, 1.0, 0.0)), -1.0).reshape(PEERS, 8, LANES)
    at8 = lax.broadcasted_iota(jnp.int32, (PEERS, 8, LANES), 1).astype(F32)
    low = jnp.where(rank8 == at8, 1.0, 0.0)
    high = jnp.where(rank8 == at8 + 8.0, 1.0, 0.0)
    map_ref[...] = jnp.concatenate([low, high], axis=1).reshape(TABLE, LANES).astype(BF16)
    eighth = jnp.full((LANES, LANES), 0.125, BF16)
    counted = sum(dot(piece, eighth, TN) for piece in split(counts8, 2))
    inverse = 1.0 / jnp.maximum(counted, 1.0)

    for copy in sends1:
        copy.wait()
    slot_map = map_ref[...]
    sums = sum(dot(slot_map, piece, TN) for piece in split(in1[...], 3))
    means = jnp.concatenate(
        [sums[:, j * LANES : (j + 1) * LANES] * inverse for j in range(width // LANES)], axis=1
    )
    means_ref[...] = means[0:CLS_DEV]
    unit = means * (1.0 / jnp.sqrt(jnp.sum(means * means, axis=1, keepdims=True) + EPSILON))
    out2[...] = sum(dot(slot_map, piece, NN) for piece in split(unit, 2))
    in2[pl.ds(0, SLOTS)] = out2[pl.ds(0, SLOTS)]
    sends2 = exchange(1, out2, in2, True)

    for copy in sends2:
        copy.wait()
    unit_high, unit_low = split(in2[...], 2)
    for n in range(rows // step):
        tile = e_ref[pl.ds(n * step, step), :]
        products = dot(unit_high, tile, NT) + dot(unit_low, tile, NT)
        slot_n = slot[:, n * step : (n + 1) * step]
        iota_n = slot_iota[:, n * step : (n + 1) * step]
        hit = slot_n == iota_n
        product = jnp.sum(jnp.where(hit, products, 0.0), axis=0, keepdims=True)
        length = jnp.sqrt(part_ref[0:1, pl.ds(n * step, step)] + EPSILON)
        mine = slot_n >= 0
        similarity = jnp.where(mine, product / length, 0.0)
        part_ref[1:2, pl.ds(n * step, step)] = similarity
        weight = jnp.where(mine, jnp.exp(SHARPNESS * (similarity - 1.0)), 0.0)
        weight = weight.astype(BF16).astype(F32)
        hot_ref[:, pl.ds(n * step, step)] = jnp.where(hit, weight, 0.0).astype(BF16)

    cut = rows // 8
    for j in range(8):
        sim_own[j : j + 1, :] = part_ref[1:2, pl.ds(j * cut, cut)]
    out3[...] = dot(hot_ref[...], e_ref[...], NN)
    in3[pl.ds(0, SLOTS)] = out3[pl.ds(0, SLOTS)]
    sends3 = exchange(2, out3, in3, False)

    spread = []
    for n, (dy, dc) in enumerate(fan):
        copy = pltpu.make_async_remote_copy(
            src_ref=sim_own,
            dst_ref=sim_in.at[n],
            send_sem=sim_ssem.at[n],
            recv_sem=sim_rsem.at[n],
            device_id=fan_device(dy, dc),
            device_id_type=MESH,
        )
        copy.start()
        spread.append(copy)
    for copy in spread:
        copy.wait()
    half = sim_own[...]
    for n in range(len(fan)):
        half = half + sim_in[n]
    sim_half[...] = half
    across = pltpu.make_async_remote_copy(
        src_ref=sim_half,
        dst_ref=sim_far,
        send_sem=sim_ssem.at[7],
        recv_sem=sim_rsem.at[7],
        device_id=far,
        device_id_type=MESH,
    )
    across.start()
    across.wait()
    both = sim_half[...] + sim_far[...]
    for j in range(8):
        sim_ref[:, pl.ds(j * cut, cut)] = both[j : j + 1, :]

    for copy in sends3:
        copy.wait()
    weighted = sum(dot(map_ref[...], piece, TN) for piece in split(in3[...], 3))
    norm = 1.0 / jnp.sqrt(jnp.sum(weighted * weighted, axis=1, keepdims=True) + EPSILON)
    proto_ref[...] = (weighted * norm)[0:CLS_DEV]


def shards(embeddings, labels, row_count):
    rows, width = embeddings.shape
    vmem = pl.BlockSpec(memory_space=pltpu.VMEM)
    table = pltpu.VMEM((TABLE, width), F32)
    line = (8, rows // 8)
    means, prototypes, similarity = pl.pallas_call(
        kernel,
        out_shape=(
            jax.ShapeDtypeStruct((CLS_DEV, width), F32),
            jax.ShapeDtypeStruct((CLS_DEV, width), F32),
            jax.ShapeDtypeStruct((1, rows), F32),
        ),
        in_specs=[
            pl.BlockSpec(memory_space=pltpu.SMEM),
            vmem,
            pl.BlockSpec(memory_space=pl.ANY),
        ],
        out_specs=(vmem, vmem, vmem),
        scratch_shapes=[
            pltpu.VMEM((rows, width), BF16),
            pltpu.VMEM((TABLE, rows), BF16),
            pltpu.VMEM((PEERS, 8, LANES), F32),
            pltpu.VMEM((PEERS, 8, LANES), F32),
            table,
            table,
            table,
            table,
            table,
            table,
            pltpu.VMEM((TABLE, LANES), BF16),
            pltpu.VMEM((8, rows), F32),
            pltpu.VMEM(line, F32),
            pltpu.VMEM((7, *line), F32),
            pltpu.VMEM(line, F32),
            pltpu.VMEM(line, F32),
            pltpu.SemaphoreType.DMA((6,)),
            pltpu.SemaphoreType.DMA((PEERS,)),
            pltpu.SemaphoreType.DMA((PEERS,)),
            pltpu.SemaphoreType.DMA((3, PEERS)),
            pltpu.SemaphoreType.DMA((3, PEERS)),
            pltpu.SemaphoreType.DMA((8,)),
            pltpu.SemaphoreType.DMA((8,)),
        ],
        compiler_params=pltpu.CompilerParams(
            collective_id=0, has_side_effects=True, vmem_limit_bytes=56 * 1024 * 1024
        ),
    )(row_count, labels.reshape(1, rows), embeddings)
    return means, prototypes, similarity.reshape(rows)


def solution(mesh):
    return jax.shard_map(
        shards,
        mesh=mesh,
        in_specs=(P("dp", None), P("dp"), P("dp")),
        out_specs=(P(("dp", "cls"), None), P(("dp", "cls"), None), P("dp")),
        check_vma=False,
    )
```

```python
import jax
import jax.numpy as jnp
from jax import lax
from jax.experimental import pallas as pl
from jax.experimental.pallas import tpu as pltpu
from jax.sharding import PartitionSpec as P

MESH = pl.DeviceIdType.MESH
F32 = jnp.float32
BF16 = jnp.bfloat16

CLS_DEV = 86
SLOTS = 16
PEERS = 16
TABLE = PEERS * SLOTS
LANES = 128
EPSILON = 1e-06
SHARPNESS = 4.0

X, Y, Z = 4, 4, 8
DX = [(0, 2, 1, 3)[k // 4] for k in range(PEERS)]
DZ = [(0, 1, -1, 2)[k % 4] for k in range(PEERS)]
HALF = PEERS // 2
GROUPS = ((7, 5, 6, 4, 3, 1, 2), (11, 15, 9, 13, 10, 14, 8, 12))
ORDER = (7, 11, 15, 5, 6, 3, 9, 13, 10, 14, 4, 8, 12, 1, 2)
CHUNK = 256
STEP = 512

NN = ((1,), (0,))
NT = ((1,), (1,))
TN = ((0,), (0,))


def split(value, parts):
    pieces, rest = [], value
    for number in range(parts):
        piece = rest.astype(BF16)
        pieces.append(piece)
        if number < parts - 1:
            rest = rest - piece.astype(F32)
    return pieces


def dot(a, b, contract):
    return lax.dot_general(a, b, (contract, ((), ())), preferred_element_type=F32)


def ranks(present):
    before = lax.broadcasted_iota(jnp.int32, (LANES, LANES), 0)
    after = lax.broadcasted_iota(jnp.int32, (LANES, LANES), 1)
    triangle = jnp.where(before < after, 1.0, 0.0).astype(BF16)
    return dot(present.astype(BF16), triangle, NN)


def kernel(
    rc_ref,
    lab_hbm,
    e_hbm,
    means_ref,
    proto_ref,
    sim_ref,
    lab_ref,
    e_ref,
    hot_ref,
    meta_out,
    meta_in,
    out1,
    in1,
    out2,
    in2,
    out3,
    in3,
    score_ref,
    map_ref,
    turned_ref,
    part_ref,
    sim_own,
    sim_in,
    sim_half,
    sim_far,
    small_sem,
    e_sem,
    meta_ssem,
    meta_rsem,
    ssem,
    rsem,
    sim_ssem,
    sim_rsem,
):
    rows, width = e_ref.shape
    chunks = width // CHUNK
    dp, cls = lax.axis_index("dp"), lax.axis_index("cls")
    x, z_lo = dp // 4, dp % 4
    y, z_hi, core = cls // 4, (cls // 2) % 2, cls % 2
    z = z_hi * 4 + z_lo
    sign = 1 - 2 * core

    def device(x_at, y_at, z_at, core_at):
        return (x_at * 4 + z_at % 4, y_at * 4 + (z_at // 4) * 2 + core_at)

    def at_offset(dx, dz):
        return device((x + X + sign * dx) % X, y, (z + Z + sign * dz) % Z, core)

    fan = [(dy, dc) for dc in range(2) for dy in range(Y) if (dy, dc) != (0, 0)]

    def fan_device(dy, dc):
        return device(x, (y + dy) % Y, z, (core + dc) % 2)

    far = device(x, y, (z + 4) % Z, core)

    smalls = [pltpu.make_async_copy(lab_hbm, lab_ref, small_sem.at[0])]
    pieces = e_sem.shape[0]
    piece_rows = rows // pieces
    loads = [
        pltpu.make_async_copy(
            e_hbm.at[pl.ds(n * piece_rows, piece_rows)],
            e_ref.at[pl.ds(n * piece_rows, piece_rows)],
            e_sem.at[n],
        )
        for n in range(pieces)
    ]
    for load in smalls + loads:
        load.start()

    barrier = pltpu.get_barrier_semaphore()
    greeted = 0
    for dx in range(X):
        for dz in range(-2, 3):
            if (dx, dz) != (0, 0):
                pl.semaphore_signal(barrier, inc=1, device_id=at_offset(dx, dz), device_id_type=MESH)
                greeted += 1
    for dy, dc in fan:
        pl.semaphore_signal(barrier, inc=1, device_id=fan_device(dy, dc), device_id_type=MESH)
        greeted += 1
    pl.semaphore_signal(barrier, inc=1, device_id=far, device_id_type=MESH)
    greeted += 1

    for load in smalls:
        load.wait()
    label = lab_ref[...]
    position = lax.broadcasted_iota(jnp.int32, (1, rows), 1)
    block = (label * 48771) >> 22
    inner = label - block * CLS_DEV
    block_dp, block_cls = block >> 4, block & 15
    block_z = ((block_cls >> 1) & 1) * 4 + (block_dp & 3)
    dx = ((block_dp >> 2) - x) * sign & 3
    dx = ((dx & 1) << 1) | (dx >> 1)
    dz = (block_z - z) * sign & 7
    turn = jnp.where(dz == 7, 2, jnp.where(dz == 2, 3, dz))
    owned = (
        (position < rc_ref[0])
        & ((block_cls >> 2) == y)
        & ((block_cls & 1) == core)
        & ((dz <= 2) | (dz == 7))
    )
    peer = jnp.where(owned, dx * 4 + turn, -1)
    peer_iota = lax.broadcasted_iota(jnp.int32, (PEERS, rows), 0)
    inner_iota = lax.broadcasted_iota(jnp.int32, (LANES, rows), 0)
    peer_hot = jnp.where(peer == peer_iota, 1.0, 0.0)
    inner_hot = jnp.where(inner == inner_iota, 1.0, 0.0).astype(BF16)
    counts = dot(peer_hot.astype(BF16), inner_hot, NT)
    rank = ranks(jnp.where(counts > 0, 1.0, 0.0))
    ranked = dot(rank.astype(BF16), inner_hot, NN)
    rank_row = jnp.sum(peer_hot * ranked, axis=0, keepdims=True)
    slot = jnp.where(owned, peer * SLOTS + rank_row.astype(jnp.int32), -1)

    for k in range(PEERS):
        meta_out[k] = jnp.broadcast_to(counts[k : k + 1], (8, LANES))
    meta_in[0] = jnp.broadcast_to(counts[0:1], (8, LANES))

    slot_iota = lax.broadcasted_iota(jnp.int32, (TABLE, STEP), 0)
    for n in range(rows // STEP):
        hit = slot[:, n * STEP : (n + 1) * STEP] == slot_iota
        hot_ref[:, pl.ds(n * STEP, STEP)] = jnp.where(hit, 1.0, 0.0).astype(BF16)

    pl.semaphore_wait(barrier, greeted)
    metas = {}
    for k in ORDER:
        metas[k] = pltpu.make_async_remote_copy(
            src_ref=meta_out.at[k],
            dst_ref=meta_in.at[k],
            send_sem=meta_ssem.at[k],
            recv_sem=meta_rsem.at[k],
            device_id=at_offset(DX[k], DZ[k]),
            device_id_type=MESH,
        )
        metas[k].start()

    moves = {}

    def send(phase, f, k):
        source, target = ((out1, in1), (out2, in2), (out3, in3))[phase]
        to = at_offset(-DX[k], -DZ[k]) if phase == 1 else at_offset(DX[k], DZ[k])
        move = pltpu.make_async_remote_copy(
            src_ref=source.at[f, pl.ds(k * SLOTS, SLOTS)],
            dst_ref=target.at[f, pl.ds(k * SLOTS, SLOTS)],
            send_sem=ssem.at[phase, f, k],
            recv_sem=rsem.at[phase, f, k],
            device_id=to,
            device_id_type=MESH,
        )
        move.start()
        moves[phase, f, k] = move

    def receive(phase, f, peers):
        for k in peers:
            moves[phase, f, k].wait_recv()

    def columns(f):
        return pl.ds(f * CHUNK, CHUNK)

    for load in loads:
        load.wait()
    for f in range(chunks):
        out1[f] = dot(hot_ref[...], e_ref[:, columns(f)], NN)
        in1[f, 0:SLOTS] = out1[f, 0:SLOTS]
        for k in ORDER:
            send(0, f, k)

    ones = jnp.ones((8, LANES), BF16)
    for n in range(rows // STEP):
        tile = e_ref[pl.ds(n * STEP, STEP), :].astype(F32)
        squares = tile * tile
        lanes = squares[:, 0:LANES]
        for j in range(1, width // LANES):
            lanes = lanes + squares[:, j * LANES : (j + 1) * LANES]
        total = sum(dot(ones, piece, NT) for piece in split(lanes, 3))
        part_ref[0:1, pl.ds(n * STEP, STEP)] = 1.0 / jnp.sqrt(total[0:1] + EPSILON)

    for k in ORDER:
        metas[k].wait()
    counts8 = meta_in[...].reshape(PEERS * 8, LANES)
    present8 = counts8 > 0
    rank8 = jnp.where(present8, ranks(jnp.where(present8, 1.0, 0.0)), -1.0).reshape(PEERS, 8, LANES)
    at8 = lax.broadcasted_iota(jnp.int32, (PEERS, 8, LANES), 1).astype(F32)
    low = jnp.where(rank8 == at8, 1.0, 0.0)
    high = jnp.where(rank8 == at8 + 8.0, 1.0, 0.0)
    slot_map = jnp.concatenate([low, high], axis=1).reshape(TABLE, LANES)
    map_ref[...] = slot_map.astype(BF16)
    turned_ref[...] = slot_map.T.astype(BF16)
    eighth = jnp.full((LANES, LANES), 0.125, BF16)
    counted = sum(dot(piece, eighth, TN) for piece in split(counts8, 2))
    inverse = 1.0 / jnp.maximum(counted, 1.0)

    for f in range(chunks):
        receive(0, f, ORDER)
        sums = sum(dot(turned_ref[...], piece, NN) for piece in split(in1[f], 3))
        means = jnp.concatenate(
            [sums[:, j * LANES : (j + 1) * LANES] * inverse for j in range(CHUNK // LANES)], axis=1
        )
        means_ref[:, columns(f)] = means[0:CLS_DEV]
        out2[f] = sum(dot(map_ref[...], piece, NN) for piece in split(means, 2))
        in2[f, 0:SLOTS] = out2[f, 0:SLOTS]
        for k in GROUPS[0]:
            send(1, f, k)
        for late in ((), (0,), (1, 2))[f]:
            for k in GROUPS[1]:
                send(1, late, k)

    def products(g, f, n):
        high, low = split(in2[f, pl.ds(g * LANES, LANES)], 2)
        both = jnp.concatenate([high, low], axis=0)
        found = dot(both, e_ref[pl.ds(n * STEP, STEP), columns(f)], NT)
        return found[0:LANES] + found[LANES:]

    def weigh(g):
        square = sum(
            jnp.sum(in2[f, pl.ds(g * LANES, LANES)] * in2[f, pl.ds(g * LANES, LANES)], axis=1, keepdims=True)
            for f in range(chunks)
        )
        scale = 1.0 / jnp.sqrt(square + EPSILON)
        iota = lax.broadcasted_iota(jnp.int32, (LANES, STEP), 0) + g * LANES
        for n in range(rows // STEP):
            at = pl.ds(n * STEP, STEP)
            score = (score_ref[g, :, at] + products(g, chunks - 1, n)) * scale
            slot_n = slot[:, n * STEP : (n + 1) * STEP]
            hit = slot_n == iota
            product = jnp.sum(jnp.where(hit, score, 0.0), axis=0, keepdims=True)
            mine = (slot_n >= g * LANES) & (slot_n < (g + 1) * LANES)
            similarity = jnp.where(mine, product * part_ref[0:1, at], 0.0)
            if g == 0:
                part_ref[1:2, at] = similarity
            else:
                part_ref[1:2, at] = part_ref[1:2, at] + similarity
            weight = jnp.where(mine, jnp.exp(SHARPNESS * (similarity - 1.0)), 0.0)
            weight = weight.astype(BF16).astype(F32)
            hot_ref[pl.ds(g * LANES, LANES), at] = jnp.where(hit, weight, 0.0).astype(BF16)

    def weighted_sums(g, f):
        own = pl.ds(g * LANES, LANES)
        out3[f, own] = dot(hot_ref[own, :], e_ref[:, columns(f)], NN)
        if g == 0:
            in3[f, 0:SLOTS] = out3[f, 0:SLOTS]
        for k in GROUPS[g]:
            send(2, f, k)

    def gather(g, f):
        receive(1, f, GROUPS[g])
        if f == chunks - 1:
            weigh(g)
        else:
            for n in range(rows // STEP):
                at = pl.ds(n * STEP, STEP)
                found = products(g, f, n)
                score_ref[g, :, at] = found if f == 0 else score_ref[g, :, at] + found

    gather(0, 0)
    gather(0, 1)
    gather(1, 0)
    gather(0, 2)
    for f in range(chunks):
        weighted_sums(0, f)
    gather(1, 1)
    gather(1, 2)

    cut = rows // 8
    for j in range(8):
        sim_own[j : j + 1, :] = part_ref[1:2, pl.ds(j * cut, cut)]
    weighted_sums(1, 0)
    spread = []
    for n, (dy, dc) in enumerate(fan):
        copy = pltpu.make_async_remote_copy(
            src_ref=sim_own,
            dst_ref=sim_in.at[n],
            send_sem=sim_ssem.at[n],
            recv_sem=sim_rsem.at[n],
            device_id=fan_device(dy, dc),
            device_id_type=MESH,
        )
        copy.start()
        spread.append(copy)
    weighted_sums(1, 1)
    weighted_sums(1, 2)
    for copy in spread:
        copy.wait()
    half = sim_own[...]
    for n in range(len(fan)):
        half = half + sim_in[n]
    sim_half[...] = half
    across = pltpu.make_async_remote_copy(
        src_ref=sim_half,
        dst_ref=sim_far,
        send_sem=sim_ssem.at[7],
        recv_sem=sim_rsem.at[7],
        device_id=far,
        device_id_type=MESH,
    )
    across.start()

    def merged(g, f):
        receive(2, f, GROUPS[g])
        own = pl.ds(g * LANES, LANES)
        return sum(dot(turned_ref[:, own], piece, NN) for piece in split(in3[f, own], 3))

    for f in range(chunks):
        score_ref[0, :, columns(f)] = merged(0, f)
    weighted = []
    for f in range(chunks):
        weighted.append(score_ref[0, :, columns(f)] + merged(1, f))
    square = sum(jnp.sum(piece * piece, axis=1, keepdims=True) for piece in weighted)
    norm = 1.0 / jnp.sqrt(square + EPSILON)
    for f in range(chunks):
        proto_ref[:, columns(f)] = (weighted[f] * norm)[0:CLS_DEV]

    across.wait()
    both = sim_half[...] + sim_far[...]
    for j in range(8):
        sim_ref[:, pl.ds(j * cut, cut)] = both[j : j + 1, :]
    for move in moves.values():
        move.wait_send()


def writer(means_ref, proto_ref, sim_ref, means_hbm, proto_hbm, sim_hbm, sem):
    copies = [
        pltpu.make_async_copy(means_ref, means_hbm, sem.at[0]),
        pltpu.make_async_copy(proto_ref, proto_hbm, sem.at[1]),
        pltpu.make_async_copy(sim_ref, sim_hbm, sem.at[2]),
    ]
    for copy in copies:
        copy.start()
    for copy in copies:
        copy.wait()


def shards(embeddings, labels, row_count):
    rows, width = embeddings.shape
    chunks = width // CHUNK
    vmem = pl.BlockSpec(memory_space=pltpu.VMEM)
    anywhere = pl.BlockSpec(memory_space=pl.ANY)
    hbm = pl.BlockSpec(memory_space=pltpu.MemorySpace.HBM)
    table = pltpu.VMEM((chunks, TABLE, CHUNK), F32)
    line = (8, rows // 8)
    shapes = ((CLS_DEV, width), (CLS_DEV, width), (1, rows))
    inputs = [row_count] + [
        pltpu.with_memory_space_constraint(a, pltpu.MemorySpace.HBM)
        for a in (labels.reshape(1, rows), embeddings)
    ]
    results = pl.pallas_call(
        kernel,
        out_shape=tuple(pltpu.VMEM(shape, F32) for shape in shapes),
        in_specs=[pl.BlockSpec(memory_space=pltpu.SMEM), hbm, hbm],
        out_specs=(vmem, vmem, vmem),
        scratch_shapes=[
            pltpu.VMEM((1, rows), jnp.int32),
            pltpu.VMEM((rows, width), BF16),
            pltpu.VMEM((TABLE, rows), BF16),
            pltpu.VMEM((PEERS, 8, LANES), F32),
            pltpu.VMEM((PEERS, 8, LANES), F32),
            table,
            table,
            table,
            table,
            table,
            table,
            pltpu.VMEM((2, LANES, rows), F32),
            pltpu.VMEM((TABLE, LANES), BF16),
            pltpu.VMEM((LANES, TABLE), BF16),
            pltpu.VMEM((8, rows), F32),
            pltpu.VMEM(line, F32),
            pltpu.VMEM((7, *line), F32),
            pltpu.VMEM(line, F32),
            pltpu.VMEM(line, F32),
            pltpu.SemaphoreType.DMA((2,)),
            pltpu.SemaphoreType.DMA((6,)),
            pltpu.SemaphoreType.DMA((PEERS,)),
            pltpu.SemaphoreType.DMA((PEERS,)),
            pltpu.SemaphoreType.DMA((3, chunks, PEERS)),
            pltpu.SemaphoreType.DMA((3, chunks, PEERS)),
            pltpu.SemaphoreType.DMA((8,)),
            pltpu.SemaphoreType.DMA((8,)),
        ],
        compiler_params=pltpu.CompilerParams(
            collective_id=0, has_side_effects=True, vmem_limit_bytes=48 * 1024 * 1024
        ),
    )(*inputs)
    results = [pltpu.with_memory_space_constraint(r, pltpu.MemorySpace.VMEM) for r in results]
    means, prototypes, similarity = pl.pallas_call(
        writer,
        out_shape=tuple(jax.ShapeDtypeStruct(shape, F32) for shape in shapes),
        in_specs=[vmem, vmem, vmem],
        out_specs=(anywhere, anywhere, anywhere),
        scratch_shapes=[pltpu.SemaphoreType.DMA((3,))],
    )(*results)
    return means, prototypes, similarity.reshape(rows)


def solution(mesh):
    return jax.shard_map(
        shards,
        mesh=mesh,
        in_specs=(P("dp", None), P("dp"), P("dp")),
        out_specs=(P(("dp", "cls"), None), P(("dp", "cls"), None), P("dp")),
        check_vma=False,
    )
```

```python
import jax
import jax.numpy as jnp
from jax import lax
from jax.experimental import pallas as pl
from jax.experimental.pallas import tpu as pltpu
from jax.sharding import PartitionSpec as P

MESH = pl.DeviceIdType.MESH
F32 = jnp.float32
BF16 = jnp.bfloat16

CLS_DEV = 86
SLOTS = 16
PEERS = 16
TABLE = PEERS * SLOTS
LANES = 128
EPSILON = 1e-06
SHARPNESS = 4.0

X, Y, Z = 4, 4, 8
DX = [(0, 2, 1, 3)[k // 4] for k in range(PEERS)]
DZ = [(0, 1, -1, 2)[k % 4] for k in range(PEERS)]
HALF = PEERS // 2
GROUPS = ((7, 5, 6, 4, 3, 1, 2), (11, 15, 9, 13, 10, 14, 8, 12))
ORDER = (7, 11, 15, 5, 6, 3, 9, 13, 10, 14, 4, 8, 12, 1, 2)
CHUNK = 256
SECOND_AT = ((), (0,), (1, 2), ())
STEP = 512

NN = ((1,), (0,))
NT = ((1,), (1,))
TN = ((0,), (0,))


def split(value, parts):
    pieces, rest = [], value
    for number in range(parts):
        piece = rest.astype(BF16)
        pieces.append(piece)
        if number < parts - 1:
            rest = rest - piece.astype(F32)
    return pieces


def dot(a, b, contract):
    return lax.dot_general(a, b, (contract, ((), ())), preferred_element_type=F32)


def ranks(present):
    before = lax.broadcasted_iota(jnp.int32, (LANES, LANES), 0)
    after = lax.broadcasted_iota(jnp.int32, (LANES, LANES), 1)
    triangle = jnp.where(before < after, 1.0, 0.0).astype(BF16)
    return dot(present.astype(BF16), triangle, NN)


def kernel(
    rc_ref,
    lab_hbm,
    e_hbm,
    means_ref,
    proto_ref,
    sim_ref,
    lab_ref,
    e_ref,
    hot_ref,
    meta_out,
    meta_in,
    out1,
    in1,
    out2,
    in2,
    out3,
    in3,
    score_ref,
    map_ref,
    turned_ref,
    part_ref,
    sim_own,
    sim_in,
    sim_half,
    sim_far,
    small_sem,
    e_sem,
    meta_ssem,
    meta_rsem,
    ssem,
    rsem,
    sim_ssem,
    sim_rsem,
):
    rows, width = e_ref.shape
    chunks = width // CHUNK
    dp, cls = lax.axis_index("dp"), lax.axis_index("cls")
    x, z_lo = dp // 4, dp % 4
    y, z_hi, core = cls // 4, (cls // 2) % 2, cls % 2
    z = z_hi * 4 + z_lo
    sign = 1 - 2 * core

    def device(x_at, y_at, z_at, core_at):
        return (x_at * 4 + z_at % 4, y_at * 4 + (z_at // 4) * 2 + core_at)

    def at_offset(dx, dz):
        return device((x + X + sign * dx) % X, y, (z + Z + sign * dz) % Z, core)

    fan = [(dy, dc) for dc in range(2) for dy in range(Y) if (dy, dc) != (0, 0)]

    def fan_device(dy, dc):
        return device(x, (y + dy) % Y, z, (core + dc) % 2)

    far = device(x, y, (z + 4) % Z, core)

    smalls = [pltpu.make_async_copy(lab_hbm, lab_ref, small_sem.at[0])]
    loads = [
        pltpu.make_async_copy(
            e_hbm.at[:, pl.ds(f * CHUNK, CHUNK)],
            e_ref.at[:, pl.ds(f * CHUNK, CHUNK)],
            e_sem.at[f],
        )
        for f in range(chunks)
    ]
    for load in smalls:
        load.start()

    barrier = pltpu.get_barrier_semaphore()
    greeted = 0
    for dx in range(X):
        for dz in range(-2, 3):
            if (dx, dz) != (0, 0):
                pl.semaphore_signal(barrier, inc=1, device_id=at_offset(dx, dz), device_id_type=MESH)
                greeted += 1
    for dy, dc in fan:
        pl.semaphore_signal(barrier, inc=1, device_id=fan_device(dy, dc), device_id_type=MESH)
        greeted += 1
    pl.semaphore_signal(barrier, inc=1, device_id=far, device_id_type=MESH)
    greeted += 1

    for load in loads:
        load.start()

    for load in smalls:
        load.wait()
    label = lab_ref[...]
    position = lax.broadcasted_iota(jnp.int32, (1, rows), 1)
    block = (label * 48771) >> 22
    inner = label - block * CLS_DEV
    block_dp, block_cls = block >> 4, block & 15
    block_z = ((block_cls >> 1) & 1) * 4 + (block_dp & 3)
    dx = ((block_dp >> 2) - x) * sign & 3
    dx = ((dx & 1) << 1) | (dx >> 1)
    dz = (block_z - z) * sign & 7
    turn = jnp.where(dz == 7, 2, jnp.where(dz == 2, 3, dz))
    owned = (
        (position < rc_ref[0])
        & ((block_cls >> 2) == y)
        & ((block_cls & 1) == core)
        & ((dz <= 2) | (dz == 7))
    )
    peer = jnp.where(owned, dx * 4 + turn, -1)
    peer_iota = lax.broadcasted_iota(jnp.int32, (PEERS, rows), 0)
    inner_iota = lax.broadcasted_iota(jnp.int32, (LANES, rows), 0)
    peer_hot = jnp.where(peer == peer_iota, 1.0, 0.0)
    inner_hot = jnp.where(inner == inner_iota, 1.0, 0.0).astype(BF16)
    counts = dot(peer_hot.astype(BF16), inner_hot, NT)
    rank = ranks(jnp.where(counts > 0, 1.0, 0.0))
    ranked = dot(rank.astype(BF16), inner_hot, NN)
    rank_row = jnp.sum(peer_hot * ranked, axis=0, keepdims=True)
    slot = jnp.where(owned, peer * SLOTS + rank_row.astype(jnp.int32), -1)

    for k in range(PEERS):
        meta_out[k] = jnp.broadcast_to(counts[k : k + 1], (8, LANES))
    meta_in[0] = jnp.broadcast_to(counts[0:1], (8, LANES))

    slot_iota = lax.broadcasted_iota(jnp.int32, (TABLE, STEP), 0)
    for n in range(rows // STEP):
        hit = slot[:, n * STEP : (n + 1) * STEP] == slot_iota
        hot_ref[:, pl.ds(n * STEP, STEP)] = jnp.where(hit, 1.0, 0.0).astype(BF16)

    moves = {}

    def send(phase, f, k):
        source, target = ((out1, in1), (out2, in2), (out3, in3))[phase]
        to = at_offset(-DX[k], -DZ[k]) if phase == 1 else at_offset(DX[k], DZ[k])
        move = pltpu.make_async_remote_copy(
            src_ref=source.at[f, pl.ds(k * SLOTS, SLOTS)],
            dst_ref=target.at[f, pl.ds(k * SLOTS, SLOTS)],
            send_sem=ssem.at[phase, f, k],
            recv_sem=rsem.at[phase, f, k],
            device_id=to,
            device_id_type=MESH,
        )
        move.start()
        moves[phase, f, k] = move

    def receive(phase, f, peers):
        for k in peers:
            moves[phase, f, k].wait_recv()

    def columns(f):
        return pl.ds(f * CHUNK, CHUNK)

    def segment_sums(slots, f):
        return dot(hot_ref[slots, :], e_ref[:, columns(f)], NN)

    loads[0].wait()
    out1[0] = segment_sums(slice(0, TABLE), 0)
    pl.semaphore_wait(barrier, greeted)
    metas = {}
    for k in ORDER:
        metas[k] = pltpu.make_async_remote_copy(
            src_ref=meta_out.at[k],
            dst_ref=meta_in.at[k],
            send_sem=meta_ssem.at[k],
            recv_sem=meta_rsem.at[k],
            device_id=at_offset(DX[k], DZ[k]),
            device_id_type=MESH,
        )
        metas[k].start()
    for f in range(chunks):
        if f > 0:
            loads[f].wait()
            out1[f] = segment_sums(slice(0, TABLE), f)
        in1[f, 0:SLOTS] = out1[f, 0:SLOTS]
        for k in ORDER:
            send(0, f, k)

    ones = jnp.ones((8, LANES), BF16)
    for n in range(rows // STEP):
        tile = e_ref[pl.ds(n * STEP, STEP), :].astype(F32)
        squares = tile * tile
        lanes = squares[:, 0:LANES]
        for j in range(1, width // LANES):
            lanes = lanes + squares[:, j * LANES : (j + 1) * LANES]
        total = sum(dot(ones, piece, NT) for piece in split(lanes, 3))
        part_ref[0:1, pl.ds(n * STEP, STEP)] = 1.0 / jnp.sqrt(total[0:1] + EPSILON)

    for k in ORDER:
        metas[k].wait()
    counts8 = meta_in[...].reshape(PEERS * 8, LANES)
    present8 = counts8 > 0
    rank8 = jnp.where(present8, ranks(jnp.where(present8, 1.0, 0.0)), -1.0).reshape(PEERS, 8, LANES)
    at8 = lax.broadcasted_iota(jnp.int32, (PEERS, 8, LANES), 1).astype(F32)
    low = jnp.where(rank8 == at8, 1.0, 0.0)
    high = jnp.where(rank8 == at8 + 8.0, 1.0, 0.0)
    slot_map = jnp.concatenate([low, high], axis=1).reshape(TABLE, LANES)
    map_ref[...] = slot_map.astype(BF16)
    turned_ref[...] = slot_map.T.astype(BF16)
    eighth = jnp.full((LANES, LANES), 0.125, BF16)
    counted = sum(dot(piece, eighth, TN) for piece in split(counts8, 2))
    inverse = 1.0 / jnp.maximum(counted, 1.0)

    for f in range(chunks):
        receive(0, f, ORDER)
        sums = sum(dot(turned_ref[...], piece, NN) for piece in split(in1[f], 3))
        means = jnp.concatenate(
            [sums[:, j * LANES : (j + 1) * LANES] * inverse for j in range(CHUNK // LANES)], axis=1
        )
        means_ref[:, columns(f)] = means[0:CLS_DEV]
        out2[f] = sum(dot(map_ref[...], piece, NN) for piece in split(means, 2))
        in2[f, 0:SLOTS] = out2[f, 0:SLOTS]
        for k in GROUPS[0]:
            send(1, f, k)
        for late in SECOND_AT[f]:
            for k in GROUPS[1]:
                send(1, late, k)

    def products(g, f, n):
        high, low = split(in2[f, pl.ds(g * LANES, LANES)], 2)
        both = jnp.concatenate([high, low], axis=0)
        found = dot(both, e_ref[pl.ds(n * STEP, STEP), columns(f)], NT)
        return found[0:LANES] + found[LANES:]

    def weigh(g):
        square = sum(
            jnp.sum(in2[f, pl.ds(g * LANES, LANES)] * in2[f, pl.ds(g * LANES, LANES)], axis=1, keepdims=True)
            for f in range(chunks)
        )
        scale = 1.0 / jnp.sqrt(square + EPSILON)
        iota = lax.broadcasted_iota(jnp.int32, (LANES, STEP), 0) + g * LANES
        for n in range(rows // STEP):
            at = pl.ds(n * STEP, STEP)
            score = (score_ref[g, :, at] + products(g, chunks - 1, n)) * scale
            slot_n = slot[:, n * STEP : (n + 1) * STEP]
            hit = slot_n == iota
            product = jnp.sum(jnp.where(hit, score, 0.0), axis=0, keepdims=True)
            mine = (slot_n >= g * LANES) & (slot_n < (g + 1) * LANES)
            similarity = jnp.where(mine, product * part_ref[0:1, at], 0.0)
            if g == 0:
                part_ref[1:2, at] = similarity
            else:
                part_ref[1:2, at] = part_ref[1:2, at] + similarity
            weight = jnp.where(mine, jnp.exp(SHARPNESS * (similarity - 1.0)), 0.0)
            weight = weight.astype(BF16).astype(F32)
            hot_ref[pl.ds(g * LANES, LANES), at] = jnp.where(hit, weight, 0.0).astype(BF16)

    def weighted_sums(g, f):
        own = slice(g * LANES, (g + 1) * LANES)
        out3[f, own] = segment_sums(own, f)
        if g == 0:
            in3[f, 0:SLOTS] = out3[f, 0:SLOTS]
        for k in GROUPS[g]:
            send(2, f, k)

    def gather(g, f):
        receive(1, f, GROUPS[g])
        if f == chunks - 1:
            weigh(g)
        else:
            for n in range(rows // STEP):
                at = pl.ds(n * STEP, STEP)
                found = products(g, f, n)
                score_ref[g, :, at] = found if f == 0 else score_ref[g, :, at] + found

    gather(0, 0)
    gather(0, 1)
    for late in SECOND_AT[chunks]:
        for k in GROUPS[1]:
            send(1, late, k)
    gather(1, 0)
    gather(0, 2)
    for f in range(chunks):
        weighted_sums(0, f)
    gather(1, 1)
    gather(1, 2)

    cut = rows // 8
    for j in range(8):
        sim_own[j : j + 1, :] = part_ref[1:2, pl.ds(j * cut, cut)]
    spread = []
    for n, (dy, dc) in enumerate(fan):
        copy = pltpu.make_async_remote_copy(
            src_ref=sim_own,
            dst_ref=sim_in.at[n],
            send_sem=sim_ssem.at[n],
            recv_sem=sim_rsem.at[n],
            device_id=fan_device(dy, dc),
            device_id_type=MESH,
        )
        copy.start()
        spread.append(copy)
    weighted_sums(1, 0)
    weighted_sums(1, 1)
    weighted_sums(1, 2)
    for copy in spread:
        copy.wait()
    half = sim_own[...]
    for n in range(len(fan)):
        half = half + sim_in[n]
    sim_half[...] = half
    across = pltpu.make_async_remote_copy(
        src_ref=sim_half,
        dst_ref=sim_far,
        send_sem=sim_ssem.at[7],
        recv_sem=sim_rsem.at[7],
        device_id=far,
        device_id_type=MESH,
    )
    across.start()

    def merged(g, f):
        receive(2, f, GROUPS[g])
        own = pl.ds(g * LANES, LANES)
        return sum(dot(turned_ref[:, own], piece, NN) for piece in split(in3[f, own], 3))

    for f in range(chunks):
        score_ref[0, :, columns(f)] = merged(0, f)
    weighted = []
    for f in range(chunks):
        weighted.append(score_ref[0, :, columns(f)] + merged(1, f))
    square = sum(jnp.sum(piece * piece, axis=1, keepdims=True) for piece in weighted)
    norm = 1.0 / jnp.sqrt(square + EPSILON)
    for f in range(chunks):
        proto_ref[:, columns(f)] = (weighted[f] * norm)[0:CLS_DEV]

    across.wait()
    both = sim_half[...] + sim_far[...]
    for j in range(8):
        sim_ref[:, pl.ds(j * cut, cut)] = both[j : j + 1, :]
    for move in moves.values():
        move.wait_send()


def writer(means_ref, proto_ref, sim_ref, means_hbm, proto_hbm, sim_hbm, sem):
    copies = [
        pltpu.make_async_copy(means_ref, means_hbm, sem.at[0]),
        pltpu.make_async_copy(proto_ref, proto_hbm, sem.at[1]),
        pltpu.make_async_copy(sim_ref, sim_hbm, sem.at[2]),
    ]
    for copy in copies:
        copy.start()
    for copy in copies:
        copy.wait()


def shards(embeddings, labels, row_count):
    rows, width = embeddings.shape
    chunks = width // CHUNK
    vmem = pl.BlockSpec(memory_space=pltpu.VMEM)
    anywhere = pl.BlockSpec(memory_space=pl.ANY)
    hbm = pl.BlockSpec(memory_space=pltpu.MemorySpace.HBM)
    table = pltpu.VMEM((chunks, TABLE, CHUNK), F32)
    line = (8, rows // 8)
    shapes = ((CLS_DEV, width), (CLS_DEV, width), (1, rows))
    inputs = [row_count] + [
        pltpu.with_memory_space_constraint(a, pltpu.MemorySpace.HBM)
        for a in (labels.reshape(1, rows), embeddings)
    ]
    results = pl.pallas_call(
        kernel,
        out_shape=tuple(pltpu.VMEM(shape, F32) for shape in shapes),
        in_specs=[pl.BlockSpec(memory_space=pltpu.SMEM), hbm, hbm],
        out_specs=(vmem, vmem, vmem),
        scratch_shapes=[
            pltpu.VMEM((1, rows), jnp.int32),
            pltpu.VMEM((rows, width), BF16),
            pltpu.VMEM((TABLE, rows), BF16),
            pltpu.VMEM((PEERS, 8, LANES), F32),
            pltpu.VMEM((PEERS, 8, LANES), F32),
            table,
            table,
            table,
            table,
            table,
            table,
            pltpu.VMEM((2, LANES, rows), F32),
            pltpu.VMEM((TABLE, LANES), BF16),
            pltpu.VMEM((LANES, TABLE), BF16),
            pltpu.VMEM((8, rows), F32),
            pltpu.VMEM(line, F32),
            pltpu.VMEM((7, *line), F32),
            pltpu.VMEM(line, F32),
            pltpu.VMEM(line, F32),
            pltpu.SemaphoreType.DMA((2,)),
            pltpu.SemaphoreType.DMA((chunks,)),
            pltpu.SemaphoreType.DMA((PEERS,)),
            pltpu.SemaphoreType.DMA((PEERS,)),
            pltpu.SemaphoreType.DMA((3, chunks, PEERS)),
            pltpu.SemaphoreType.DMA((3, chunks, PEERS)),
            pltpu.SemaphoreType.DMA((8,)),
            pltpu.SemaphoreType.DMA((8,)),
        ],
        compiler_params=pltpu.CompilerParams(
            collective_id=0, has_side_effects=True, vmem_limit_bytes=48 * 1024 * 1024
        ),
    )(*inputs)
    results = [pltpu.with_memory_space_constraint(r, pltpu.MemorySpace.VMEM) for r in results]
    means, prototypes, similarity = pl.pallas_call(
        writer,
        out_shape=tuple(jax.ShapeDtypeStruct(shape, F32) for shape in shapes),
        in_specs=[vmem, vmem, vmem],
        out_specs=(anywhere, anywhere, anywhere),
        scratch_shapes=[pltpu.SemaphoreType.DMA((3,))],
    )(*results)
    return means, prototypes, similarity.reshape(rows)


def solution(mesh):
    return jax.shard_map(
        shards,
        mesh=mesh,
        in_specs=(P("dp", None), P("dp"), P("dp")),
        out_specs=(P(("dp", "cls"), None), P(("dp", "cls"), None), P("dp")),
        check_vma=False,
    )
```

```python
import jax
import jax.numpy as jnp
from jax import lax
from jax.experimental import pallas as pl
from jax.experimental.pallas import tpu as pltpu
from jax.sharding import PartitionSpec as P

MESH = pl.DeviceIdType.MESH
F32 = jnp.float32
BF16 = jnp.bfloat16

CLS_DEV = 86
SLOTS = 16
PEERS = 16
TABLE = PEERS * SLOTS
LANES = 128
EPSILON = 1e-06
SHARPNESS = 4.0

X, Y, Z = 4, 4, 8
DX = [(0, 2, 1, 3)[k // 4] for k in range(PEERS)]
DZ = [(0, 1, -1, 2)[k % 4] for k in range(PEERS)]
HALF = PEERS // 2
GROUPS = ((7, 5, 6, 4, 3, 1, 2), (11, 15, 9, 13, 10, 14, 8, 12))
ORDER = (7, 11, 15, 5, 6, 3, 9, 13, 10, 14, 4, 8, 12, 1, 2)
CUTS = (0, 256, 512, 768)
CUTS3 = (0, 256, 768)
SECOND_AT = ((), (0,), (1, 2))
TAKE = ((0, 0), (0, 1), (1, 0), (0, 2))
TAKE_LATE = ((1, 1), (1, 2))
STEP = 512

NN = ((1,), (0,))
NT = ((1,), (1,))
TN = ((0,), (0,))


def split(value, parts):
    pieces, rest = [], value
    for number in range(parts):
        piece = rest.astype(BF16)
        pieces.append(piece)
        if number < parts - 1:
            rest = rest - piece.astype(F32)
    return pieces


def dot(a, b, contract):
    return lax.dot_general(a, b, (contract, ((), ())), preferred_element_type=F32)


def ranks(present):
    before = lax.broadcasted_iota(jnp.int32, (LANES, LANES), 0)
    after = lax.broadcasted_iota(jnp.int32, (LANES, LANES), 1)
    triangle = jnp.where(before < after, 1.0, 0.0).astype(BF16)
    return dot(present.astype(BF16), triangle, NN)


def kernel(
    rc_ref,
    lab_hbm,
    e_hbm,
    means_ref,
    proto_ref,
    sim_ref,
    lab_ref,
    e_ref,
    hot_ref,
    meta_out,
    meta_in,
    out1,
    in1,
    out2,
    in2,
    out3,
    in3,
    score_ref,
    map_ref,
    turned_ref,
    part_ref,
    sim_own,
    sim_in,
    sim_half,
    sim_far,
    small_sem,
    e_sem,
    meta_ssem,
    meta_rsem,
    ssem,
    rsem,
    sim_ssem,
    sim_rsem,
):
    rows, width = e_ref.shape
    chunks, chunks3 = len(CUTS) - 1, len(CUTS3) - 1
    dp, cls = lax.axis_index("dp"), lax.axis_index("cls")
    x, z_lo = dp // 4, dp % 4
    y, z_hi, core = cls // 4, (cls // 2) % 2, cls % 2
    z = z_hi * 4 + z_lo
    sign = 1 - 2 * core

    def device(x_at, y_at, z_at, core_at):
        return (x_at * 4 + z_at % 4, y_at * 4 + (z_at // 4) * 2 + core_at)

    def at_offset(dx, dz):
        return device((x + X + sign * dx) % X, y, (z + Z + sign * dz) % Z, core)

    fan = [(dy, dc) for dc in range(2) for dy in range(Y) if (dy, dc) != (0, 0)]

    def fan_device(dy, dc):
        return device(x, (y + dy) % Y, z, (core + dc) % 2)

    far = device(x, y, (z + 4) % Z, core)

    def columns(f, cuts=CUTS):
        return slice(cuts[f], cuts[f + 1])

    smalls = [pltpu.make_async_copy(lab_hbm, lab_ref, small_sem.at[0])]
    loads = [
        pltpu.make_async_copy(
            e_hbm.at[:, columns(f)],
            e_ref.at[:, columns(f)],
            e_sem.at[f],
        )
        for f in range(chunks)
    ]
    for load in smalls:
        load.start()

    barrier = pltpu.get_barrier_semaphore()
    plane = [(dx, dz) for dx in range(X) for dz in range(-2, 3) if (dx, dz) != (0, 0)]
    plane.sort(key=lambda at: -min(at[0], X - at[0]) - abs(at[1]))
    greeted = [far] + [at_offset(*at) for at in plane] + [fan_device(*at) for at in fan]
    for other in greeted:
        pl.semaphore_signal(barrier, inc=1, device_id=other, device_id_type=MESH)
    for load in loads:
        load.start()

    for load in smalls:
        load.wait()
    label = lab_ref[...]
    position = lax.broadcasted_iota(jnp.int32, (1, rows), 1)
    block = (label * 48771) >> 22
    inner = label - block * CLS_DEV
    block_dp, block_cls = block >> 4, block & 15
    block_z = ((block_cls >> 1) & 1) * 4 + (block_dp & 3)
    dx = ((block_dp >> 2) - x) * sign & 3
    dx = ((dx & 1) << 1) | (dx >> 1)
    dz = (block_z - z) * sign & 7
    turn = jnp.where(dz == 7, 2, jnp.where(dz == 2, 3, dz))
    owned = (
        (position < rc_ref[0])
        & ((block_cls >> 2) == y)
        & ((block_cls & 1) == core)
        & ((dz <= 2) | (dz == 7))
    )
    peer = jnp.where(owned, dx * 4 + turn, -1)
    peer_iota = lax.broadcasted_iota(jnp.int32, (PEERS, rows), 0)
    inner_iota = lax.broadcasted_iota(jnp.int32, (LANES, rows), 0)
    peer_hot = jnp.where(peer == peer_iota, 1.0, 0.0)
    inner_hot = jnp.where(inner == inner_iota, 1.0, 0.0).astype(BF16)
    counts = dot(peer_hot.astype(BF16), inner_hot, NT)
    rank = ranks(jnp.where(counts > 0, 1.0, 0.0))
    ranked = dot(rank.astype(BF16), inner_hot, NN)
    rank_row = jnp.sum(peer_hot * ranked, axis=0, keepdims=True)
    slot = jnp.where(owned, peer * SLOTS + rank_row.astype(jnp.int32), -1)

    for k in range(PEERS):
        meta_out[k] = counts[k : k + 1]
    meta_in[0] = counts[0:1]

    slot_iota = lax.broadcasted_iota(jnp.int32, (TABLE, STEP), 0)
    for n in range(rows // STEP):
        hit = slot[:, n * STEP : (n + 1) * STEP] == slot_iota
        hot_ref[:, pl.ds(n * STEP, STEP)] = jnp.where(hit, 1.0, 0.0).astype(BF16)

    moves = {}

    def send(phase, f, k):
        source, target = ((out1, in1), (out2, in2), (out3, in3))[phase]
        to = at_offset(-DX[k], -DZ[k]) if phase == 1 else at_offset(DX[k], DZ[k])
        move = pltpu.make_async_remote_copy(
            src_ref=source.at[pl.ds(k * SLOTS, SLOTS), columns(f, CUTS3 if phase == 2 else CUTS)],
            dst_ref=target.at[pl.ds(k * SLOTS, SLOTS), columns(f, CUTS3 if phase == 2 else CUTS)],
            send_sem=ssem.at[phase, f, k],
            recv_sem=rsem.at[phase, f, k],
            device_id=to,
            device_id_type=MESH,
        )
        move.start()
        moves[phase, f, k] = move

    def receive(phase, f, peers):
        for k in peers:
            moves[phase, f, k].wait_recv()

    def segment_sums(slots, f, cuts=CUTS):
        return dot(hot_ref[slots, :], e_ref[:, columns(f, cuts)], NN)

    loads[0].wait()
    out1[:, columns(0)] = segment_sums(slice(0, TABLE), 0)
    pl.semaphore_wait(barrier, len(greeted))
    for f in range(chunks):
        if f > 0:
            loads[f].wait()
            out1[:, columns(f)] = segment_sums(slice(0, TABLE), f)
        in1[0:SLOTS, columns(f)] = out1[0:SLOTS, columns(f)]
        for k in ORDER:
            send(0, f, k)
        if f == 0:
            metas = {}
            for k in ORDER:
                metas[k] = pltpu.make_async_remote_copy(
                    src_ref=meta_out.at[k],
                    dst_ref=meta_in.at[k],
                    send_sem=meta_ssem.at[k],
                    recv_sem=meta_rsem.at[k],
                    device_id=at_offset(DX[k], DZ[k]),
                    device_id_type=MESH,
                )
                metas[k].start()

    ones = jnp.ones((8, LANES), BF16)
    for n in range(rows // STEP):
        tile = e_ref[pl.ds(n * STEP, STEP), :].astype(F32)
        squares = tile * tile
        lanes = squares[:, 0:LANES]
        for j in range(1, width // LANES):
            lanes = lanes + squares[:, j * LANES : (j + 1) * LANES]
        total = sum(dot(ones, piece, NT) for piece in split(lanes, 3))
        part_ref[0:1, pl.ds(n * STEP, STEP)] = 1.0 / jnp.sqrt(total[0:1] + EPSILON)

    for k in ORDER:
        metas[k].wait()
    counts8 = jnp.concatenate([jnp.broadcast_to(meta_in[k], (8, LANES)) for k in range(PEERS)], axis=0)
    present8 = counts8 > 0
    rank8 = jnp.where(present8, ranks(jnp.where(present8, 1.0, 0.0)), -1.0).reshape(PEERS, 8, LANES)
    at8 = lax.broadcasted_iota(jnp.int32, (PEERS, 8, LANES), 1).astype(F32)
    low = jnp.where(rank8 == at8, 1.0, 0.0)
    high = jnp.where(rank8 == at8 + 8.0, 1.0, 0.0)
    slot_map = jnp.concatenate([low, high], axis=1).reshape(TABLE, LANES)
    map_ref[...] = slot_map.astype(BF16)
    turned_ref[...] = slot_map.T.astype(BF16)
    eighth = jnp.full((LANES, LANES), 0.125, BF16)
    counted = sum(dot(piece, eighth, TN) for piece in split(counts8, 2))
    inverse = 1.0 / jnp.maximum(counted, 1.0)

    for f in range(chunks):
        receive(0, f, ORDER)
        sums = sum(dot(turned_ref[...], piece, NN) for piece in split(in1[:, columns(f)], 3))
        means = jnp.concatenate(
            [sums[:, j * LANES : (j + 1) * LANES] * inverse for j in range(sums.shape[1] // LANES)], axis=1
        )
        means_ref[:, columns(f)] = means[0:CLS_DEV]
        out2[:, columns(f)] = sum(dot(map_ref[...], piece, NN) for piece in split(means, 2))
        in2[0:SLOTS, columns(f)] = out2[0:SLOTS, columns(f)]
        for k in GROUPS[0]:
            send(1, f, k)
        for late in SECOND_AT[f]:
            for k in GROUPS[1]:
                send(1, late, k)

    def products(g, f, n):
        high, low = split(in2[pl.ds(g * LANES, LANES), columns(f)], 2)
        both = jnp.concatenate([high, low], axis=0)
        found = dot(both, e_ref[pl.ds(n * STEP, STEP), columns(f)], NT)
        return found[0:LANES] + found[LANES:]

    def weigh(g):
        means = in2[pl.ds(g * LANES, LANES), :]
        square = jnp.sum(means * means, axis=1, keepdims=True)
        scale = 1.0 / jnp.sqrt(square + EPSILON)
        iota = lax.broadcasted_iota(jnp.int32, (LANES, STEP), 0) + g * LANES
        for n in range(rows // STEP):
            at = pl.ds(n * STEP, STEP)
            score = (score_ref[g, :, at] + products(g, chunks - 1, n)) * scale
            slot_n = slot[:, n * STEP : (n + 1) * STEP]
            hit = slot_n == iota
            product = jnp.sum(jnp.where(hit, score, 0.0), axis=0, keepdims=True)
            mine = (slot_n >= g * LANES) & (slot_n < (g + 1) * LANES)
            similarity = jnp.where(mine, product * part_ref[0:1, at], 0.0)
            if g == 0:
                part_ref[1:2, at] = similarity
            else:
                part_ref[1:2, at] = part_ref[1:2, at] + similarity
            weight = jnp.where(mine, jnp.exp(SHARPNESS * (similarity - 1.0)), 0.0)
            weight = weight.astype(BF16).astype(F32)
            hot_ref[pl.ds(g * LANES, LANES), at] = jnp.where(hit, weight, 0.0).astype(BF16)

    def weighted_sums(g, f):
        own = slice(g * LANES, (g + 1) * LANES)
        out3[own, columns(f, CUTS3)] = segment_sums(own, f, CUTS3)
        if g == 0:
            in3[0:SLOTS, columns(f, CUTS3)] = out3[0:SLOTS, columns(f, CUTS3)]
        for k in GROUPS[g]:
            send(2, f, k)

    def gather(g, f):
        receive(1, f, GROUPS[g])
        if f == chunks - 1:
            weigh(g)
        else:
            for n in range(rows // STEP):
                at = pl.ds(n * STEP, STEP)
                found = products(g, f, n)
                score_ref[g, :, at] = found if f == 0 else score_ref[g, :, at] + found

    for g, f in TAKE:
        gather(g, f)
    for f in range(chunks3):
        weighted_sums(0, f)
    for g, f in TAKE_LATE:
        gather(g, f)

    cut = rows // 8
    for j in range(8):
        sim_own[j : j + 1, :] = part_ref[1:2, pl.ds(j * cut, cut)]
    spread = []
    for n, (dy, dc) in enumerate(fan):
        copy = pltpu.make_async_remote_copy(
            src_ref=sim_own,
            dst_ref=sim_in.at[n],
            send_sem=sim_ssem.at[n],
            recv_sem=sim_rsem.at[n],
            device_id=fan_device(dy, dc),
            device_id_type=MESH,
        )
        copy.start()
        spread.append(copy)
    for f in range(chunks3):
        weighted_sums(1, f)
    for copy in spread:
        copy.wait()
    half = sim_own[...]
    for n in range(len(fan)):
        half = half + sim_in[n]
    sim_half[...] = half
    across = pltpu.make_async_remote_copy(
        src_ref=sim_half,
        dst_ref=sim_far,
        send_sem=sim_ssem.at[7],
        recv_sem=sim_rsem.at[7],
        device_id=far,
        device_id_type=MESH,
    )
    across.start()

    for (phase, f, k), move in moves.items():
        if phase < 2:
            move.wait_send()

    def merged(g, f):
        receive(2, f, GROUPS[g])
        own = pl.ds(g * LANES, LANES)
        return sum(dot(turned_ref[:, own], piece, NN) for piece in split(in3[own, columns(f, CUTS3)], 3))

    for f in range(chunks3):
        score_ref[0, :, columns(f, CUTS3)] = merged(0, f)
    weighted = []
    for f in range(chunks3):
        weighted.append(score_ref[0, :, columns(f, CUTS3)] + merged(1, f))
    square = sum(jnp.sum(piece * piece, axis=1, keepdims=True) for piece in weighted)
    norm = 1.0 / jnp.sqrt(square + EPSILON)
    for f in range(chunks3):
        proto_ref[:, columns(f, CUTS3)] = (weighted[f] * norm)[0:CLS_DEV]

    across.wait()
    both = sim_half[...] + sim_far[...]
    for j in range(8):
        sim_ref[:, pl.ds(j * cut, cut)] = both[j : j + 1, :]
    for (phase, f, k), move in moves.items():
        if phase == 2:
            move.wait_send()


def writer(means_ref, proto_ref, sim_ref, means_hbm, proto_hbm, sim_hbm, sem):
    copies = [
        pltpu.make_async_copy(means_ref, means_hbm, sem.at[0]),
        pltpu.make_async_copy(proto_ref, proto_hbm, sem.at[1]),
        pltpu.make_async_copy(sim_ref, sim_hbm, sem.at[2]),
    ]
    for copy in copies:
        copy.start()
    for copy in copies:
        copy.wait()


def shards(embeddings, labels, row_count):
    rows, width = embeddings.shape
    chunks = max(len(CUTS), len(CUTS3)) - 1
    vmem = pl.BlockSpec(memory_space=pltpu.VMEM)
    anywhere = pl.BlockSpec(memory_space=pl.ANY)
    hbm = pl.BlockSpec(memory_space=pltpu.MemorySpace.HBM)
    table = pltpu.VMEM((TABLE, width), F32)
    line = (8, rows // 8)
    shapes = ((CLS_DEV, width), (CLS_DEV, width), (1, rows))
    inputs = [row_count] + [
        pltpu.with_memory_space_constraint(a, pltpu.MemorySpace.HBM)
        for a in (labels.reshape(1, rows), embeddings)
    ]
    results = pl.pallas_call(
        kernel,
        out_shape=tuple(pltpu.VMEM(shape, F32) for shape in shapes),
        in_specs=[pl.BlockSpec(memory_space=pltpu.SMEM), hbm, hbm],
        out_specs=(vmem, vmem, vmem),
        scratch_shapes=[
            pltpu.VMEM((1, rows), jnp.int32),
            pltpu.VMEM((rows, width), BF16),
            pltpu.VMEM((TABLE, rows), BF16),
            pltpu.VMEM((PEERS, 1, LANES), F32),
            pltpu.VMEM((PEERS, 1, LANES), F32),
            table,
            table,
            table,
            table,
            table,
            table,
            pltpu.VMEM((2, LANES, rows), F32),
            pltpu.VMEM((TABLE, LANES), BF16),
            pltpu.VMEM((LANES, TABLE), BF16),
            pltpu.VMEM((8, rows), F32),
            pltpu.VMEM(line, F32),
            pltpu.VMEM((7, *line), F32),
            pltpu.VMEM(line, F32),
            pltpu.VMEM(line, F32),
            pltpu.SemaphoreType.DMA((2,)),
            pltpu.SemaphoreType.DMA((chunks,)),
            pltpu.SemaphoreType.DMA((PEERS,)),
            pltpu.SemaphoreType.DMA((PEERS,)),
            pltpu.SemaphoreType.DMA((3, chunks, PEERS)),
            pltpu.SemaphoreType.DMA((3, chunks, PEERS)),
            pltpu.SemaphoreType.DMA((8,)),
            pltpu.SemaphoreType.DMA((8,)),
        ],
        compiler_params=pltpu.CompilerParams(
            collective_id=0, has_side_effects=True, vmem_limit_bytes=48 * 1024 * 1024
        ),
    )(*inputs)
    results = [pltpu.with_memory_space_constraint(r, pltpu.MemorySpace.VMEM) for r in results]
    means, prototypes, similarity = pl.pallas_call(
        writer,
        out_shape=tuple(jax.ShapeDtypeStruct(shape, F32) for shape in shapes),
        in_specs=[vmem, vmem, vmem],
        out_specs=(anywhere, anywhere, anywhere),
        scratch_shapes=[pltpu.SemaphoreType.DMA((3,))],
    )(*results)
    return means, prototypes, similarity.reshape(rows)


def solution(mesh):
    return jax.shard_map(
        shards,
        mesh=mesh,
        in_specs=(P("dp", None), P("dp"), P("dp")),
        out_specs=(P(("dp", "cls"), None), P(("dp", "cls"), None), P("dp")),
        check_vma=False,
    )
```

```python
import jax
import jax.numpy as jnp
from jax import lax
from jax.experimental import pallas as pl
from jax.experimental.pallas import tpu as pltpu
from jax.sharding import PartitionSpec as P

MESH = pl.DeviceIdType.MESH
F32 = jnp.float32
BF16 = jnp.bfloat16

CLS_DEV = 86
SLOTS = 16
PEERS = 16
TABLE = PEERS * SLOTS
LANES = 128
EPSILON = 1e-06
SHARPNESS = 4.0

X, Y, Z = 4, 4, 8
DX = [(0, 2, 1, 3)[k // 4] for k in range(PEERS)]
DZ = [(0, 1, -1, 2)[k % 4] for k in range(PEERS)]
HALF = PEERS // 2
GROUPS = ((7, 5, 6, 4, 3, 1, 2), (11, 15, 9, 13, 10, 14, 8, 12))
ORDER = (7, 11, 15, 5, 6, 3, 9, 13, 10, 14, 4, 8, 12, 1, 2)
CUTS = (0, 256, 512, 768)
CUTS3 = (0, 256, 768)
SECOND_AT = ((), (0,), (1, 2))
TAKE = ((0, 0), (0, 1), (1, 0), (0, 2))
TAKE_LATE = ((1, 1), (1, 2))
STEP = 512

NN = ((1,), (0,))
NT = ((1,), (1,))
TN = ((0,), (0,))


def split(value, parts):
    pieces, rest = [], value
    for number in range(parts):
        piece = rest.astype(BF16)
        pieces.append(piece)
        if number < parts - 1:
            rest = rest - piece.astype(F32)
    return pieces


def dot(a, b, contract):
    return lax.dot_general(a, b, (contract, ((), ())), preferred_element_type=F32)


def ranks(present):
    before = lax.broadcasted_iota(jnp.int32, (LANES, LANES), 0)
    after = lax.broadcasted_iota(jnp.int32, (LANES, LANES), 1)
    triangle = jnp.where(before < after, 1.0, 0.0).astype(BF16)
    return dot(present.astype(BF16), triangle, NN)


def kernel(
    rc_ref,
    lab_hbm,
    e_hbm,
    means_ref,
    proto_ref,
    sim_ref,
    lab_ref,
    e_ref,
    hot_ref,
    meta_out,
    meta_in,
    out1,
    in1,
    out2,
    in2,
    out3,
    in3,
    score_ref,
    map_ref,
    turned_ref,
    part_ref,
    sim_own,
    sim_in,
    sim_half,
    sim_far,
    small_sem,
    e_sem,
    meta_ssem,
    meta_rsem,
    ssem,
    rsem,
    sim_ssem,
    sim_rsem,
):
    rows, width = e_ref.shape
    chunks, chunks3 = len(CUTS) - 1, len(CUTS3) - 1
    dp, cls = lax.axis_index("dp"), lax.axis_index("cls")
    x, z_lo = dp // 4, dp % 4
    y, z_hi, core = cls // 4, (cls // 2) % 2, cls % 2
    z = z_hi * 4 + z_lo
    sign = 1 - 2 * core

    def device(x_at, y_at, z_at, core_at):
        return (x_at * 4 + z_at % 4, y_at * 4 + (z_at // 4) * 2 + core_at)

    def at_offset(dx, dz):
        return device((x + X + sign * dx) % X, y, (z + Z + sign * dz) % Z, core)

    fan = [(dy, dc) for dc in range(2) for dy in range(Y) if (dy, dc) != (0, 0)]

    def fan_device(dy, dc):
        return device(x, (y + dy) % Y, z, (core + dc) % 2)

    far = device(x, y, (z + 4) % Z, core)

    def columns(f, cuts=CUTS):
        return slice(cuts[f], cuts[f + 1])

    smalls = [pltpu.make_async_copy(lab_hbm, lab_ref, small_sem.at[0])]
    loads = [
        pltpu.make_async_copy(
            e_hbm.at[:, columns(f)],
            e_ref.at[:, columns(f)],
            e_sem.at[f],
        )
        for f in range(chunks)
    ]
    for load in smalls:
        load.start()

    barrier = pltpu.get_barrier_semaphore()
    plane = [(dx, dz) for dx in range(X) for dz in range(-2, 3) if (dx, dz) != (0, 0)]
    plane.sort(key=lambda at: -min(at[0], X - at[0]) - abs(at[1]))
    greeted = [far] + [at_offset(*at) for at in plane] + [fan_device(*at) for at in fan]
    for other in greeted:
        pl.semaphore_signal(barrier, inc=1, device_id=other, device_id_type=MESH)
    for load in loads:
        load.start()

    for load in smalls:
        load.wait()
    label = lab_ref[...]
    position = lax.broadcasted_iota(jnp.int32, (1, rows), 1)
    block = (label * 48771) >> 22
    inner = label - block * CLS_DEV
    block_dp, block_cls = block >> 4, block & 15
    block_z = ((block_cls >> 1) & 1) * 4 + (block_dp & 3)
    dx = ((block_dp >> 2) - x) * sign & 3
    dx = ((dx & 1) << 1) | (dx >> 1)
    dz = (block_z - z) * sign & 7
    turn = jnp.where(dz == 7, 2, jnp.where(dz == 2, 3, dz))
    owned = (
        (position < rc_ref[0])
        & ((block_cls >> 2) == y)
        & ((block_cls & 1) == core)
        & ((dz <= 2) | (dz == 7))
    )
    peer = jnp.where(owned, dx * 4 + turn, -1)
    peer_iota = lax.broadcasted_iota(jnp.int32, (PEERS, rows), 0)
    inner_iota = lax.broadcasted_iota(jnp.int32, (LANES, rows), 0)
    peer_hot = jnp.where(peer == peer_iota, 1.0, 0.0)
    inner_hot = jnp.where(inner == inner_iota, 1.0, 0.0).astype(BF16)
    counts = dot(peer_hot.astype(BF16), inner_hot, NT)
    rank = ranks(jnp.where(counts > 0, 1.0, 0.0))
    ranked = dot(rank.astype(BF16), inner_hot, NN)
    rank_row = jnp.sum(peer_hot * ranked, axis=0, keepdims=True)
    slot = jnp.where(owned, peer * SLOTS + rank_row.astype(jnp.int32), -1)

    for k in range(PEERS):
        meta_out[k] = counts[k : k + 1]
    meta_in[0] = counts[0:1]

    slot_iota = lax.broadcasted_iota(jnp.int32, (TABLE, STEP), 0)
    for n in range(rows // STEP):
        hit = slot[:, n * STEP : (n + 1) * STEP] == slot_iota
        hot_ref[:, pl.ds(n * STEP, STEP)] = jnp.where(hit, 1.0, 0.0).astype(BF16)

    def send(phase, f, k):
        source, target = ((out1, in1), (out2, in2), (out3, in3))[phase]
        to = at_offset(-DX[k], -DZ[k]) if phase == 1 else at_offset(DX[k], DZ[k])
        move = pltpu.make_async_remote_copy(
            src_ref=source.at[pl.ds(k * SLOTS, SLOTS), columns(f, CUTS3 if phase == 2 else CUTS)],
            dst_ref=target.at[pl.ds(k * SLOTS, SLOTS), columns(f, CUTS3 if phase == 2 else CUTS)],
            send_sem=ssem.at[phase, f, k // HALF],
            recv_sem=rsem.at[phase, f, k // HALF],
            device_id=to,
            device_id_type=MESH,
        )
        move.start()

    def all_of(sem, array, phase, f, g):
        first = max(g * HALF, 1) * SLOTS
        span = array.at[first : (g + 1) * HALF * SLOTS, columns(f, CUTS3 if phase == 2 else CUTS)]
        pltpu.make_async_copy(span, span, sem.at[phase, f, g]).wait()

    def receive(phase, f, g):
        all_of(rsem, (in1, in2, in3)[phase], phase, f, g)

    def sent(phases):
        for phase in phases:
            for f in range(chunks3 if phase == 2 else chunks):
                for g in range(2):
                    all_of(ssem, (out1, out2, out3)[phase], phase, f, g)

    def segment_sums(slots, f, cuts=CUTS):
        return dot(hot_ref[slots, :], e_ref[:, columns(f, cuts)], NN)

    loads[0].wait()
    out1[:, columns(0)] = segment_sums(slice(0, TABLE), 0)
    pl.semaphore_wait(barrier, len(greeted))
    for f in range(chunks):
        if f > 0:
            loads[f].wait()
            out1[:, columns(f)] = segment_sums(slice(0, TABLE), f)
        in1[0:SLOTS, columns(f)] = out1[0:SLOTS, columns(f)]
        for k in ORDER:
            send(0, f, k)
        if f == 0:
            metas = {}
            for k in ORDER:
                metas[k] = pltpu.make_async_remote_copy(
                    src_ref=meta_out.at[k],
                    dst_ref=meta_in.at[k],
                    send_sem=meta_ssem.at[0],
                    recv_sem=meta_rsem.at[0],
                    device_id=at_offset(DX[k], DZ[k]),
                    device_id_type=MESH,
                )
                metas[k].start()

    ones = jnp.ones((8, LANES), BF16)
    for n in range(rows // STEP):
        tile = e_ref[pl.ds(n * STEP, STEP), :].astype(F32)
        squares = tile * tile
        lanes = squares[:, 0:LANES]
        for j in range(1, width // LANES):
            lanes = lanes + squares[:, j * LANES : (j + 1) * LANES]
        total = sum(dot(ones, piece, NT) for piece in split(lanes, 3))
        part_ref[0:1, pl.ds(n * STEP, STEP)] = 1.0 / jnp.sqrt(total[0:1] + EPSILON)

    for sem, array in ((meta_ssem, meta_out), (meta_rsem, meta_in)):
        span = array.at[1:PEERS]
        pltpu.make_async_copy(span, span, sem.at[0]).wait()
    counts8 = jnp.concatenate([jnp.broadcast_to(meta_in[k], (8, LANES)) for k in range(PEERS)], axis=0)
    present8 = counts8 > 0
    rank8 = jnp.where(present8, ranks(jnp.where(present8, 1.0, 0.0)), -1.0).reshape(PEERS, 8, LANES)
    at8 = lax.broadcasted_iota(jnp.int32, (PEERS, 8, LANES), 1).astype(F32)
    low = jnp.where(rank8 == at8, 1.0, 0.0)
    high = jnp.where(rank8 == at8 + 8.0, 1.0, 0.0)
    slot_map = jnp.concatenate([low, high], axis=1).reshape(TABLE, LANES)
    map_ref[...] = slot_map.astype(BF16)
    turned_ref[...] = slot_map.T.astype(BF16)
    eighth = jnp.full((LANES, LANES), 0.125, BF16)
    counted = sum(dot(piece, eighth, TN) for piece in split(counts8, 2))
    inverse = 1.0 / jnp.maximum(counted, 1.0)

    for f in range(chunks):
        receive(0, f, 0)
        receive(0, f, 1)
        sums = sum(dot(turned_ref[...], piece, NN) for piece in split(in1[:, columns(f)], 3))
        means = jnp.concatenate(
            [sums[:, j * LANES : (j + 1) * LANES] * inverse for j in range(sums.shape[1] // LANES)], axis=1
        )
        means_ref[:, columns(f)] = means[0:CLS_DEV]
        out2[:, columns(f)] = sum(dot(map_ref[...], piece, NN) for piece in split(means, 2))
        in2[0:SLOTS, columns(f)] = out2[0:SLOTS, columns(f)]
        for k in GROUPS[0]:
            send(1, f, k)
        for late in SECOND_AT[f]:
            for k in GROUPS[1]:
                send(1, late, k)

    def products(g, f, n):
        high, low = split(in2[pl.ds(g * LANES, LANES), columns(f)], 2)
        both = jnp.concatenate([high, low], axis=0)
        found = dot(both, e_ref[pl.ds(n * STEP, STEP), columns(f)], NT)
        return found[0:LANES] + found[LANES:]

    def weigh(g):
        means = in2[pl.ds(g * LANES, LANES), :]
        square = jnp.sum(means * means, axis=1, keepdims=True)
        scale = 1.0 / jnp.sqrt(square + EPSILON)
        iota = lax.broadcasted_iota(jnp.int32, (LANES, STEP), 0) + g * LANES
        for n in range(rows // STEP):
            at = pl.ds(n * STEP, STEP)
            score = (score_ref[g, :, at] + products(g, chunks - 1, n)) * scale
            slot_n = slot[:, n * STEP : (n + 1) * STEP]
            hit = slot_n == iota
            product = jnp.sum(jnp.where(hit, score, 0.0), axis=0, keepdims=True)
            mine = (slot_n >= g * LANES) & (slot_n < (g + 1) * LANES)
            similarity = jnp.where(mine, product * part_ref[0:1, at], 0.0)
            if g == 0:
                part_ref[1:2, at] = similarity
            else:
                part_ref[1:2, at] = part_ref[1:2, at] + similarity
            weight = jnp.where(mine, jnp.exp(SHARPNESS * (similarity - 1.0)), 0.0)
            weight = weight.astype(BF16).astype(F32)
            hot_ref[pl.ds(g * LANES, LANES), at] = jnp.where(hit, weight, 0.0).astype(BF16)

    def weighted_sums(g, f):
        own = slice(g * LANES, (g + 1) * LANES)
        out3[own, columns(f, CUTS3)] = segment_sums(own, f, CUTS3)
        if g == 0:
            in3[0:SLOTS, columns(f, CUTS3)] = out3[0:SLOTS, columns(f, CUTS3)]
        for k in GROUPS[g]:
            send(2, f, k)

    def gather(g, f):
        receive(1, f, g)
        if f == chunks - 1:
            weigh(g)
        else:
            for n in range(rows // STEP):
                at = pl.ds(n * STEP, STEP)
                found = products(g, f, n)
                score_ref[g, :, at] = found if f == 0 else score_ref[g, :, at] + found

    for g, f in TAKE:
        gather(g, f)
    for f in range(chunks3):
        weighted_sums(0, f)
    for g, f in TAKE_LATE:
        gather(g, f)

    cut = rows // 8
    for j in range(8):
        sim_own[j : j + 1, :] = part_ref[1:2, pl.ds(j * cut, cut)]
    spread = []
    for n, (dy, dc) in enumerate(fan):
        copy = pltpu.make_async_remote_copy(
            src_ref=sim_own,
            dst_ref=sim_in.at[n],
            send_sem=sim_ssem.at[n],
            recv_sem=sim_rsem.at[n],
            device_id=fan_device(dy, dc),
            device_id_type=MESH,
        )
        copy.start()
        spread.append(copy)
    for f in range(chunks3):
        weighted_sums(1, f)
    for copy in spread:
        copy.wait()
    half = sim_own[...]
    for n in range(len(fan)):
        half = half + sim_in[n]
    sim_half[...] = half
    across = pltpu.make_async_remote_copy(
        src_ref=sim_half,
        dst_ref=sim_far,
        send_sem=sim_ssem.at[7],
        recv_sem=sim_rsem.at[7],
        device_id=far,
        device_id_type=MESH,
    )
    across.start()

    sent((0, 1))

    def merged(g, f):
        receive(2, f, g)
        own = pl.ds(g * LANES, LANES)
        return sum(dot(turned_ref[:, own], piece, NN) for piece in split(in3[own, columns(f, CUTS3)], 3))

    for f in range(chunks3):
        score_ref[0, :, columns(f, CUTS3)] = merged(0, f)
    weighted = []
    for f in range(chunks3):
        weighted.append(score_ref[0, :, columns(f, CUTS3)] + merged(1, f))
    square = sum(jnp.sum(piece * piece, axis=1, keepdims=True) for piece in weighted)
    norm = 1.0 / jnp.sqrt(square + EPSILON)
    for f in range(chunks3):
        proto_ref[:, columns(f, CUTS3)] = (weighted[f] * norm)[0:CLS_DEV]

    across.wait()
    both = sim_half[...] + sim_far[...]
    for j in range(8):
        sim_ref[:, pl.ds(j * cut, cut)] = both[j : j + 1, :]
    sent((2,))


def writer(means_ref, proto_ref, sim_ref, means_hbm, proto_hbm, sim_hbm, sem):
    copies = [
        pltpu.make_async_copy(means_ref, means_hbm, sem.at[0]),
        pltpu.make_async_copy(proto_ref, proto_hbm, sem.at[1]),
        pltpu.make_async_copy(sim_ref, sim_hbm, sem.at[2]),
    ]
    for copy in copies:
        copy.start()
    for copy in copies:
        copy.wait()


def shards(embeddings, labels, row_count):
    rows, width = embeddings.shape
    chunks = max(len(CUTS), len(CUTS3)) - 1
    vmem = pl.BlockSpec(memory_space=pltpu.VMEM)
    anywhere = pl.BlockSpec(memory_space=pl.ANY)
    hbm = pl.BlockSpec(memory_space=pltpu.MemorySpace.HBM)
    table = pltpu.VMEM((TABLE, width), F32)
    line = (8, rows // 8)
    shapes = ((CLS_DEV, width), (CLS_DEV, width), (1, rows))
    inputs = [row_count] + [
        pltpu.with_memory_space_constraint(a, pltpu.MemorySpace.HBM)
        for a in (labels.reshape(1, rows), embeddings)
    ]
    results = pl.pallas_call(
        kernel,
        out_shape=tuple(pltpu.VMEM(shape, F32) for shape in shapes),
        in_specs=[pl.BlockSpec(memory_space=pltpu.SMEM), hbm, hbm],
        out_specs=(vmem, vmem, vmem),
        scratch_shapes=[
            pltpu.VMEM((1, rows), jnp.int32),
            pltpu.VMEM((rows, width), BF16),
            pltpu.VMEM((TABLE, rows), BF16),
            pltpu.VMEM((PEERS, 1, LANES), F32),
            pltpu.VMEM((PEERS, 1, LANES), F32),
            table,
            table,
            table,
            table,
            table,
            table,
            pltpu.VMEM((2, LANES, rows), F32),
            pltpu.VMEM((TABLE, LANES), BF16),
            pltpu.VMEM((LANES, TABLE), BF16),
            pltpu.VMEM((8, rows), F32),
            pltpu.VMEM(line, F32),
            pltpu.VMEM((7, *line), F32),
            pltpu.VMEM(line, F32),
            pltpu.VMEM(line, F32),
            pltpu.SemaphoreType.DMA((2,)),
            pltpu.SemaphoreType.DMA((chunks,)),
            pltpu.SemaphoreType.DMA((1,)),
            pltpu.SemaphoreType.DMA((1,)),
            pltpu.SemaphoreType.DMA((3, chunks, 2)),
            pltpu.SemaphoreType.DMA((3, chunks, 2)),
            pltpu.SemaphoreType.DMA((8,)),
            pltpu.SemaphoreType.DMA((8,)),
        ],
        compiler_params=pltpu.CompilerParams(
            collective_id=0, has_side_effects=True, vmem_limit_bytes=48 * 1024 * 1024
        ),
    )(*inputs)
    results = [pltpu.with_memory_space_constraint(r, pltpu.MemorySpace.VMEM) for r in results]
    means, prototypes, similarity = pl.pallas_call(
        writer,
        out_shape=tuple(jax.ShapeDtypeStruct(shape, F32) for shape in shapes),
        in_specs=[vmem, vmem, vmem],
        out_specs=(anywhere, anywhere, anywhere),
        scratch_shapes=[pltpu.SemaphoreType.DMA((3,))],
    )(*results)
    return means, prototypes, similarity.reshape(rows)


def solution(mesh):
    return jax.shard_map(
        shards,
        mesh=mesh,
        in_specs=(P("dp", None), P("dp"), P("dp")),
        out_specs=(P(("dp", "cls"), None), P(("dp", "cls"), None), P("dp")),
        check_vma=False,
    )
```

```python
import jax
import jax.numpy as jnp
from jax import lax
from jax.experimental import pallas as pl
from jax.experimental.pallas import tpu as pltpu
from jax.sharding import PartitionSpec as P

MESH = pl.DeviceIdType.MESH
F32 = jnp.float32
BF16 = jnp.bfloat16

CLS_DEV = 86
SLOTS = 16
PEERS = 16
TABLE = PEERS * SLOTS
LANES = 128
EPSILON = 1e-06
SHARPNESS = 4.0

X, Y, Z = 4, 4, 8
DX = [(0, 2, 1, 3)[k // 4] for k in range(PEERS)]
DZ = [(0, 1, -1, 2)[k % 4] for k in range(PEERS)]
HALF = PEERS // 2
GROUPS = ((7, 5, 6, 4, 3, 1, 2), (11, 15, 9, 13, 10, 14, 8, 12))
ORDER = (7, 11, 15, 5, 6, 3, 9, 13, 10, 14, 4, 8, 12, 1, 2)
CUTS = (0, 256, 512, 768)
CUTS3 = (0, 256, 768)
SECOND_AT = ((), (0,), (1, 2))
TAKE = ((0, 0), (0, 1), (1, 0), (0, 2))
TAKE_LATE = ((1, 1), (1, 2))
STEP = 512

NN = ((1,), (0,))
NT = ((1,), (1,))
TN = ((0,), (0,))


def split(value, parts):
    pieces, rest = [], value
    for number in range(parts):
        piece = rest.astype(BF16)
        pieces.append(piece)
        if number < parts - 1:
            rest = rest - piece.astype(F32)
    return pieces


def dot(a, b, contract):
    return lax.dot_general(a, b, (contract, ((), ())), preferred_element_type=F32)


def ranks(present):
    before = lax.broadcasted_iota(jnp.int32, (LANES, LANES), 0)
    after = lax.broadcasted_iota(jnp.int32, (LANES, LANES), 1)
    triangle = jnp.where(before < after, 1.0, 0.0).astype(BF16)
    return dot(present.astype(BF16), triangle, NN)


def kernel(
    rc_ref,
    lab_hbm,
    e_hbm,
    means_ref,
    proto_ref,
    sim_ref,
    lab_ref,
    e_ref,
    hot_ref,
    meta_out,
    meta_in,
    out1,
    in1,
    out2,
    in2,
    out3,
    in3,
    score_ref,
    map_ref,
    turned_ref,
    part_ref,
    sim_own,
    sim_in,
    sim_half,
    sim_far,
    small_sem,
    e_sem,
    meta_ssem,
    meta_rsem,
    ssem,
    rsem,
    sim_ssem,
    sim_rsem,
):
    rows, width = e_ref.shape
    chunks, chunks3 = len(CUTS) - 1, len(CUTS3) - 1
    dp, cls = lax.axis_index("dp"), lax.axis_index("cls")
    x, z_lo = dp // 4, dp % 4
    y, z_hi, core = cls // 4, (cls // 2) % 2, cls % 2
    z = z_hi * 4 + z_lo
    sign = 1 - 2 * core

    def device(x_at, y_at, z_at, core_at):
        return (x_at * 4 + z_at % 4, y_at * 4 + (z_at // 4) * 2 + core_at)

    def at_offset(dx, dz):
        return device((x + X + sign * dx) % X, y, (z + Z + sign * dz) % Z, core)

    fan = [(dy, dc) for dc in range(2) for dy in range(Y) if (dy, dc) != (0, 0)]

    def fan_device(dy, dc):
        return device(x, (y + dy) % Y, z, (core + dc) % 2)

    far = device(x, y, (z + 4) % Z, core)

    def columns(f, cuts=CUTS):
        return slice(cuts[f], cuts[f + 1])

    smalls = [pltpu.make_async_copy(lab_hbm, lab_ref, small_sem.at[0])]
    loads = [
        pltpu.make_async_copy(
            e_hbm.at[:, columns(f)],
            e_ref.at[:, columns(f)],
            e_sem.at[f],
        )
        for f in range(chunks)
    ]
    for load in smalls:
        load.start()

    barrier = pltpu.get_barrier_semaphore()
    plane = [(dx, dz) for dx in range(X) for dz in range(-2, 3) if (dx, dz) != (0, 0)]
    plane.sort(key=lambda at: -min(at[0], X - at[0]) - abs(at[1]))
    greeted = [far] + [at_offset(*at) for at in plane] + [fan_device(*at) for at in fan]
    for other in greeted:
        pl.semaphore_signal(barrier, inc=1, device_id=other, device_id_type=MESH)
    for load in loads:
        load.start()

    for load in smalls:
        load.wait()
    label = lab_ref[...]
    position = lax.broadcasted_iota(jnp.int32, (1, rows), 1)
    block = (label * 48771) >> 22
    inner = label - block * CLS_DEV
    block_dp, block_cls = block >> 4, block & 15
    block_z = ((block_cls >> 1) & 1) * 4 + (block_dp & 3)
    dx = ((block_dp >> 2) - x) * sign & 3
    dx = ((dx & 1) << 1) | (dx >> 1)
    dz = (block_z - z) * sign & 7
    turn = jnp.where(dz == 7, 2, jnp.where(dz == 2, 3, dz))
    owned = (
        (position < rc_ref[0])
        & ((block_cls >> 2) == y)
        & ((block_cls & 1) == core)
        & ((dz <= 2) | (dz == 7))
    )
    peer = jnp.where(owned, dx * 4 + turn, -1)
    peer_iota = lax.broadcasted_iota(jnp.int32, (PEERS, rows), 0)
    inner_iota = lax.broadcasted_iota(jnp.int32, (LANES, rows), 0)
    peer_hot = jnp.where(peer == peer_iota, 1.0, 0.0)
    inner_hot = jnp.where(inner == inner_iota, 1.0, 0.0).astype(BF16)
    counts = dot(peer_hot.astype(BF16), inner_hot, NT)
    rank = ranks(jnp.where(counts > 0, 1.0, 0.0))
    ranked = dot(rank.astype(BF16), inner_hot, NN)
    rank_row = jnp.sum(peer_hot * ranked, axis=0, keepdims=True)
    slot = jnp.where(owned, peer * SLOTS + rank_row.astype(jnp.int32), -1)

    for k in range(PEERS):
        meta_out[k] = counts[k : k + 1]
    meta_in[0] = counts[0:1]

    slot_iota = lax.broadcasted_iota(jnp.int32, (TABLE, STEP), 0)
    for n in range(rows // STEP):
        hit = slot[:, n * STEP : (n + 1) * STEP] == slot_iota
        hot_ref[:, pl.ds(n * STEP, STEP)] = jnp.where(hit, 1.0, 0.0).astype(BF16)

    def send(phase, f, k):
        source, target = ((out1, in1), (out2, in2), (out3, in3))[phase]
        to = at_offset(-DX[k], -DZ[k]) if phase == 1 else at_offset(DX[k], DZ[k])
        move = pltpu.make_async_remote_copy(
            src_ref=source.at[pl.ds(k * SLOTS, SLOTS), columns(f, CUTS3 if phase == 2 else CUTS)],
            dst_ref=target.at[pl.ds(k * SLOTS, SLOTS), columns(f, CUTS3 if phase == 2 else CUTS)],
            send_sem=ssem.at[phase, f, k // HALF],
            recv_sem=rsem.at[phase, f, k // HALF],
            device_id=to,
            device_id_type=MESH,
        )
        move.start()

    def all_of(sem, array, phase, f, g):
        first = max(g * HALF, 1) * SLOTS
        span = array.at[first : (g + 1) * HALF * SLOTS, columns(f, CUTS3 if phase == 2 else CUTS)]
        pltpu.make_async_copy(span, span, sem.at[phase, f, g]).wait()

    def receive(phase, f, g):
        all_of(rsem, (in1, in2, in3)[phase], phase, f, g)

    def sent(phases):
        for phase in phases:
            for f in range(chunks3 if phase == 2 else chunks):
                for g in range(2):
                    all_of(ssem, (out1, out2, out3)[phase], phase, f, g)

    def segment_sums(slots, f, cuts=CUTS):
        return dot(hot_ref[slots, :], e_ref[:, columns(f, cuts)], NN)

    loads[0].wait()
    out1[:, columns(0)] = segment_sums(slice(0, TABLE), 0)
    pl.semaphore_wait(barrier, len(greeted))
    for f in range(chunks):
        if f > 0:
            loads[f].wait()
            out1[:, columns(f)] = segment_sums(slice(0, TABLE), f)
        in1[0:SLOTS, columns(f)] = out1[0:SLOTS, columns(f)]
        for k in ORDER:
            send(0, f, k)
        if f == 0:
            metas = {}
            for k in ORDER:
                metas[k] = pltpu.make_async_remote_copy(
                    src_ref=meta_out.at[k],
                    dst_ref=meta_in.at[k],
                    send_sem=meta_ssem.at[0],
                    recv_sem=meta_rsem.at[0],
                    device_id=at_offset(DX[k], DZ[k]),
                    device_id_type=MESH,
                )
                metas[k].start()

    ones = jnp.ones((8, LANES), BF16)
    for n in range(rows // STEP):
        tile = e_ref[pl.ds(n * STEP, STEP), :].astype(F32)
        squares = tile * tile
        lanes = squares[:, 0:LANES]
        for j in range(1, width // LANES):
            lanes = lanes + squares[:, j * LANES : (j + 1) * LANES]
        total = sum(dot(ones, piece, NT) for piece in split(lanes, 3))
        part_ref[0:1, pl.ds(n * STEP, STEP)] = 1.0 / jnp.sqrt(total[0:1] + EPSILON)

    for sem, array in ((meta_ssem, meta_out), (meta_rsem, meta_in)):
        span = array.at[1:PEERS]
        pltpu.make_async_copy(span, span, sem.at[0]).wait()
    counts8 = jnp.concatenate([jnp.broadcast_to(meta_in[k], (8, LANES)) for k in range(PEERS)], axis=0)
    present8 = counts8 > 0
    rank8 = jnp.where(present8, ranks(jnp.where(present8, 1.0, 0.0)), -1.0).reshape(PEERS, 8, LANES)
    at8 = lax.broadcasted_iota(jnp.int32, (PEERS, 8, LANES), 1).astype(F32)
    low = jnp.where(rank8 == at8, 1.0, 0.0)
    high = jnp.where(rank8 == at8 + 8.0, 1.0, 0.0)
    slot_map = jnp.concatenate([low, high], axis=1).reshape(TABLE, LANES)
    map_ref[...] = slot_map.astype(BF16)
    turned_ref[...] = slot_map.T.astype(BF16)
    eighth = jnp.full((LANES, LANES), 0.125, BF16)
    counted = sum(dot(piece, eighth, TN) for piece in split(counts8, 2))
    inverse = 1.0 / jnp.maximum(counted, 1.0)

    for f in range(chunks):
        receive(0, f, 0)
        receive(0, f, 1)
        sums = sum(dot(turned_ref[...], piece, NN) for piece in split(in1[:, columns(f)], 3))
        means = jnp.concatenate(
            [sums[:, j * LANES : (j + 1) * LANES] * inverse for j in range(sums.shape[1] // LANES)], axis=1
        )
        means_ref[:, columns(f)] = means[0:CLS_DEV]
        out2[:, columns(f)] = sum(dot(map_ref[...], piece, NN) for piece in split(means, 2))
        in2[0:SLOTS, columns(f)] = out2[0:SLOTS, columns(f)]
        for k in GROUPS[0]:
            send(1, f, k)
        for late in SECOND_AT[f]:
            for k in GROUPS[1]:
                send(1, late, k)

    def products(g, f, n):
        high, low = split(in2[pl.ds(g * LANES, LANES), columns(f)], 2)
        both = jnp.concatenate([high, low], axis=0)
        found = dot(both, e_ref[pl.ds(n * STEP, STEP), columns(f)], NT)
        return found[0:LANES] + found[LANES:]

    def weigh(g):
        means = in2[pl.ds(g * LANES, LANES), :]
        square = jnp.sum(means * means, axis=1, keepdims=True)
        scale = 1.0 / jnp.sqrt(square + EPSILON)
        iota = lax.broadcasted_iota(jnp.int32, (LANES, STEP), 0) + g * LANES
        for n in range(rows // STEP):
            at = pl.ds(n * STEP, STEP)
            score = (score_ref[g, :, at] + products(g, chunks - 1, n)) * scale
            slot_n = slot[:, n * STEP : (n + 1) * STEP]
            hit = slot_n == iota
            product = jnp.sum(jnp.where(hit, score, 0.0), axis=0, keepdims=True)
            mine = (slot_n >= g * LANES) & (slot_n < (g + 1) * LANES)
            similarity = jnp.where(mine, product * part_ref[0:1, at], 0.0)
            if g == 0:
                part_ref[1:2, at] = similarity
            else:
                part_ref[1:2, at] = part_ref[1:2, at] + similarity
            weight = jnp.where(mine, jnp.exp(SHARPNESS * (similarity - 1.0)), 0.0)
            weight = weight.astype(BF16).astype(F32)
            hot_ref[pl.ds(g * LANES, LANES), at] = jnp.where(hit, weight, 0.0).astype(BF16)

    def weighted_sums(g, f):
        own = slice(g * LANES, (g + 1) * LANES)
        out3[own, columns(f, CUTS3)] = segment_sums(own, f, CUTS3)
        if g == 0:
            in3[0:SLOTS, columns(f, CUTS3)] = out3[0:SLOTS, columns(f, CUTS3)]
        for k in GROUPS[g]:
            send(2, f, k)

    def gather(g, f):
        receive(1, f, g)
        if f == chunks - 1:
            weigh(g)
        else:
            for n in range(rows // STEP):
                at = pl.ds(n * STEP, STEP)
                found = products(g, f, n)
                score_ref[g, :, at] = found if f == 0 else score_ref[g, :, at] + found

    for g, f in TAKE:
        gather(g, f)
    for f in range(chunks3):
        weighted_sums(0, f)
    for g, f in TAKE_LATE:
        gather(g, f)

    cut = rows // 8
    for j in range(8):
        sim_own[j : j + 1, :] = part_ref[1:2, pl.ds(j * cut, cut)]
    for n, (dy, dc) in enumerate(fan):
        copy = pltpu.make_async_remote_copy(
            src_ref=sim_own,
            dst_ref=sim_in.at[n],
            send_sem=sim_ssem.at[0],
            recv_sem=sim_rsem.at[0],
            device_id=fan_device(dy, dc),
            device_id_type=MESH,
        )
        copy.start()
    for f in range(chunks3):
        weighted_sums(1, f)
    for sem in (sim_ssem, sim_rsem):
        pltpu.make_async_copy(sim_in, sim_in, sem.at[0]).wait()
    half = sim_own[...]
    for n in range(len(fan)):
        half = half + sim_in[n]
    sim_half[...] = half
    across = pltpu.make_async_remote_copy(
        src_ref=sim_half,
        dst_ref=sim_far,
        send_sem=sim_ssem.at[1],
        recv_sem=sim_rsem.at[1],
        device_id=far,
        device_id_type=MESH,
    )
    across.start()

    sent((0, 1))

    def merged(g, f):
        receive(2, f, g)
        own = pl.ds(g * LANES, LANES)
        return sum(dot(turned_ref[:, own], piece, NN) for piece in split(in3[own, columns(f, CUTS3)], 3))

    for f in range(chunks3):
        score_ref[0, :, columns(f, CUTS3)] = merged(0, f)
    weighted = []
    for f in range(chunks3):
        weighted.append(score_ref[0, :, columns(f, CUTS3)] + merged(1, f))
    square = sum(jnp.sum(piece * piece, axis=1, keepdims=True) for piece in weighted)
    norm = 1.0 / jnp.sqrt(square + EPSILON)
    for f in range(chunks3):
        proto_ref[:, columns(f, CUTS3)] = (weighted[f] * norm)[0:CLS_DEV]

    across.wait()
    both = sim_half[...] + sim_far[...]
    for j in range(8):
        sim_ref[:, pl.ds(j * cut, cut)] = both[j : j + 1, :]
    sent((2,))


def writer(means_ref, proto_ref, sim_ref, means_hbm, proto_hbm, sim_hbm, sem):
    copies = [
        pltpu.make_async_copy(means_ref, means_hbm, sem.at[0]),
        pltpu.make_async_copy(proto_ref, proto_hbm, sem.at[1]),
        pltpu.make_async_copy(sim_ref, sim_hbm, sem.at[2]),
    ]
    for copy in copies:
        copy.start()
    for copy in copies:
        copy.wait()


def shards(embeddings, labels, row_count):
    rows, width = embeddings.shape
    chunks = max(len(CUTS), len(CUTS3)) - 1
    vmem = pl.BlockSpec(memory_space=pltpu.VMEM)
    anywhere = pl.BlockSpec(memory_space=pl.ANY)
    hbm = pl.BlockSpec(memory_space=pltpu.MemorySpace.HBM)
    table = pltpu.VMEM((TABLE, width), F32)
    line = (8, rows // 8)
    shapes = ((CLS_DEV, width), (CLS_DEV, width), (1, rows))
    inputs = [row_count] + [
        pltpu.with_memory_space_constraint(a, pltpu.MemorySpace.HBM)
        for a in (labels.reshape(1, rows), embeddings)
    ]
    results = pl.pallas_call(
        kernel,
        out_shape=tuple(pltpu.VMEM(shape, F32) for shape in shapes),
        in_specs=[pl.BlockSpec(memory_space=pltpu.SMEM), hbm, hbm],
        out_specs=(vmem, vmem, vmem),
        scratch_shapes=[
            pltpu.VMEM((1, rows), jnp.int32),
            pltpu.VMEM((rows, width), BF16),
            pltpu.VMEM((TABLE, rows), BF16),
            pltpu.VMEM((PEERS, 1, LANES), F32),
            pltpu.VMEM((PEERS, 1, LANES), F32),
            table,
            table,
            table,
            table,
            table,
            table,
            pltpu.VMEM((2, LANES, rows), F32),
            pltpu.VMEM((TABLE, LANES), BF16),
            pltpu.VMEM((LANES, TABLE), BF16),
            pltpu.VMEM((8, rows), F32),
            pltpu.VMEM(line, F32),
            pltpu.VMEM((7, *line), F32),
            pltpu.VMEM(line, F32),
            pltpu.VMEM(line, F32),
            pltpu.SemaphoreType.DMA((2,)),
            pltpu.SemaphoreType.DMA((chunks,)),
            pltpu.SemaphoreType.DMA((1,)),
            pltpu.SemaphoreType.DMA((1,)),
            pltpu.SemaphoreType.DMA((3, chunks, 2)),
            pltpu.SemaphoreType.DMA((3, chunks, 2)),
            pltpu.SemaphoreType.DMA((2,)),
            pltpu.SemaphoreType.DMA((2,)),
        ],
        compiler_params=pltpu.CompilerParams(
            collective_id=0, has_side_effects=True, vmem_limit_bytes=48 * 1024 * 1024
        ),
    )(*inputs)
    results = [pltpu.with_memory_space_constraint(r, pltpu.MemorySpace.VMEM) for r in results]
    means, prototypes, similarity = pl.pallas_call(
        writer,
        out_shape=tuple(jax.ShapeDtypeStruct(shape, F32) for shape in shapes),
        in_specs=[vmem, vmem, vmem],
        out_specs=(anywhere, anywhere, anywhere),
        scratch_shapes=[pltpu.SemaphoreType.DMA((3,))],
    )(*results)
    return means, prototypes, similarity.reshape(rows)


def solution(mesh):
    return jax.shard_map(
        shards,
        mesh=mesh,
        in_specs=(P("dp", None), P("dp"), P("dp")),
        out_specs=(P(("dp", "cls"), None), P(("dp", "cls"), None), P("dp")),
        check_vma=False,
    )
```
